16 devices in a mesh: dp: 2 (over y, z), seq: 8 (over x, core).
Axes of the slice: x: 4, y: 2, z: 1, core: 2. Of those that a mesh axis runs over, the one named last changes fastest.
The devices are a block of a 4x4x8 slice.
Arguments:
- enc_out: bfloat16 [128, 64, 512], P('dp', 'seq'), parts along dimension 0
- pred_out: bfloat16 [128, 8, 640], P('dp'), parts along dimension 0
- w_enc: bfloat16 [512, 640], replicated
- w_pred: bfloat16 [640, 640], replicated
- w_out: bfloat16 [640, 1024], replicated
- labels: int32 [128, 7], P('dp'), parts along dimension 0
- frame_len: int32 [128], P('dp'), parts along dimension 0
- label_len: int32 [128], P('dp'), parts along dimension 0
Outputs:
- output 1: float32 [128], P('dp'), parts along dimension 0
- output 2: bfloat16 [128, 64, 512], P('dp', 'seq'), parts along dimension 0
- output 3: float32 [1024, 640], P('dp'), parts along dimension 0
- output 4: float32 [1280, 640], P('dp'), parts along dimension 0
- output 5: float32 [1280, 1024], P('dp'), parts along dimension 0
There are 2 independent parts. The reference program is written for one: setup_inputs(seed, part) draws one part's arguments, and reference() takes and returns one part's arrays. A program takes and returns all parts, laid end to end along the dimension named above; an argument that names none is the same for every part.
All inputs are finite; a program needn't handle non-finite values.
Results may differ from the reference program's by a relative error of at most 0.0139293.
Values are sent between devices in bfloat16 or wider.
A program may use at most 768 MiB of HBM per device.

```python
import jax
import jax.numpy as jnp
from jax import lax

NUM_UTT = 64
NUM_FRAMES = 64
LABEL_POS = 8
ENC_DIM = 512
PRED_DIM = 640
JOINT_DIM = 640
VOCAB_SIZE = 1024
FRAME_BLOCK = 8
NUM_LABELS = LABEL_POS - 1
NUM_BLOCKS = NUM_FRAMES // FRAME_BLOCK
NEG_FILL = -1.0e30


def setup_inputs(seed: int = 0, part: int = 0) -> dict:
    shared_key, part_base = jax.random.split(jax.random.key(seed))
    part_key = jax.random.fold_in(part_base, part)
    k_enc, k_pred, k_lab, k_frames, k_lens = jax.random.split(part_key, 5)
    k_wenc, k_wpred, k_wout = jax.random.split(shared_key, 3)
    enc_out = jax.random.normal(k_enc, (NUM_UTT, NUM_FRAMES, ENC_DIM), jnp.float32).astype(jnp.bfloat16)
    pred_out = jax.random.normal(k_pred, (NUM_UTT, LABEL_POS, PRED_DIM), jnp.float32).astype(jnp.bfloat16)
    w_enc = (jax.random.normal(k_wenc, (ENC_DIM, JOINT_DIM), jnp.float32) * ENC_DIM ** -0.5).astype(jnp.bfloat16)
    w_pred = (jax.random.normal(k_wpred, (PRED_DIM, JOINT_DIM), jnp.float32) * PRED_DIM ** -0.5).astype(jnp.bfloat16)
    w_out = (jax.random.normal(k_wout, (JOINT_DIM, VOCAB_SIZE), jnp.float32) * (1.5 * JOINT_DIM ** -0.5)).astype(jnp.bfloat16)
    labels = jax.random.randint(k_lab, (NUM_UTT, NUM_LABELS), 1, VOCAB_SIZE, jnp.int32)
    frame_len = jax.random.randint(k_frames, (NUM_UTT,), NUM_FRAMES // 4 + 1, NUM_FRAMES + 1, jnp.int32).at[0].set(NUM_FRAMES)
    label_len = jax.random.randint(k_lens, (NUM_UTT,), 1, NUM_LABELS + 1, jnp.int32).at[NUM_UTT - 1].set(NUM_LABELS)
    return {'enc_out': enc_out, 'pred_out': pred_out, 'w_enc': w_enc, 'w_pred': w_pred, 'w_out': w_out, 'labels': labels, 'frame_len': frame_len, 'label_len': label_len}


def joint_block(enc_blk, act_g, w_enc, w_out):
    n_utt, n_blk, _ = enc_blk.shape
    act_f = jnp.dot(enc_blk.reshape(n_utt * n_blk, ENC_DIM), w_enc, preferred_element_type=jnp.float32).astype(jnp.bfloat16).reshape(n_utt, n_blk, JOINT_DIM)
    hidden = jnp.tanh(act_f[:, :, None, :].astype(jnp.float32) + act_g[:, None, :, :].astype(jnp.float32)).astype(jnp.bfloat16)
    logits = jnp.dot(hidden.reshape(n_utt * n_blk * LABEL_POS, JOINT_DIM), w_out, preferred_element_type=jnp.float32).reshape(n_utt, n_blk, LABEL_POS, VOCAB_SIZE)
    return hidden, jax.nn.log_softmax(logits, axis=-1)


def label_prefix(frame_lab):
    zero_col = jnp.zeros_like(frame_lab[:, :1])
    return jnp.concatenate([zero_col, jnp.cumsum(frame_lab, axis=1)], axis=1)


def reference(enc_out, pred_out, w_enc, w_pred, w_out, labels, frame_len, label_len):
    act_g = jnp.dot(pred_out.reshape(NUM_UTT * LABEL_POS, PRED_DIM), w_pred, preferred_element_type=jnp.float32).astype(jnp.bfloat16).reshape(NUM_UTT, LABEL_POS, JOINT_DIM)
    lab_ids = jnp.concatenate([labels, jnp.full((NUM_UTT, 1), -1, jnp.int32)], axis=1)
    lab_index = jnp.broadcast_to(labels[:, None, :, None], (NUM_UTT, FRAME_BLOCK, NUM_LABELS, 1))
    enc_blocks = enc_out.reshape(NUM_UTT, NUM_BLOCKS, FRAME_BLOCK, ENC_DIM).transpose(1, 0, 2, 3)

    def lattice_scores(enc_blk):
        _, log_probs = joint_block(enc_blk, act_g, w_enc, w_out)
        lab_lp = jnp.take_along_axis(log_probs[:, :, :NUM_LABELS, :], lab_index, axis=3)[..., 0]
        return log_probs[..., 0], lab_lp

    blank_blocks, lab_blocks = lax.map(lattice_scores, enc_blocks)
    blank_lp = blank_blocks.transpose(1, 0, 2, 3).reshape(NUM_UTT, NUM_FRAMES, LABEL_POS)
    lab_lp = lab_blocks.transpose(1, 0, 2, 3).reshape(NUM_UTT, NUM_FRAMES, NUM_LABELS)

    pos_ids = jnp.arange(LABEL_POS)[None, :]
    neg_rows = jnp.full((NUM_UTT, LABEL_POS), NEG_FILL, jnp.float32)
    init_x = jnp.where(pos_ids == 0, 0.0, neg_rows)
    boundary = jnp.where(pos_ids == label_len[:, None], 0.0, neg_rows)

    def alpha_step(x_prev, frame_in):
        frame_blank, frame_lab = frame_in
        lab_sum = label_prefix(frame_lab)
        alpha_t = lab_sum + lax.cumlogsumexp(x_prev - lab_sum, axis=1)
        return alpha_t + frame_blank, alpha_t

    _, alphas = lax.scan(alpha_step, init_x, (blank_lp.transpose(1, 0, 2), lab_lp.transpose(1, 0, 2)))
    alphas = alphas.transpose(1, 0, 2)

    def beta_step(next_row, frame_in):
        frame_blank, frame_lab, frame_id = frame_in
        lab_sum = label_prefix(frame_lab)
        beta_row = lax.cumlogsumexp(next_row + frame_blank + lab_sum, axis=1, reverse=True) - lab_sum
        beta_row = jnp.where((frame_id >= frame_len)[:, None], boundary, beta_row)
        return beta_row, (beta_row, next_row)

    first_row, (betas, beta_next) = lax.scan(beta_step, boundary, (blank_lp.transpose(1, 0, 2), lab_lp.transpose(1, 0, 2), jnp.arange(NUM_FRAMES)), reverse=True)
    betas = betas.transpose(1, 0, 2)
    beta_next = beta_next.transpose(1, 0, 2)
    log_prob = first_row[:, 0]

    beta_up = jnp.concatenate([betas[:, :, 1:], jnp.full((NUM_UTT, NUM_FRAMES, 1), NEG_FILL, jnp.float32)], axis=2)
    lab_full = jnp.concatenate([lab_lp, jnp.zeros((NUM_UTT, NUM_FRAMES, 1), jnp.float32)], axis=2)
    frame_ok = (jnp.arange(NUM_FRAMES)[None, :] < frame_len[:, None])[:, :, None]
    norm_shift = log_prob[:, None, None]
    occ_blank = jnp.where(frame_ok, jnp.exp(jnp.minimum(alphas + blank_lp + beta_next - norm_shift, 0.0)), 0.0)
    occ_lab = jnp.where(frame_ok, jnp.exp(jnp.minimum(alphas + lab_full + beta_up - norm_shift, 0.0)), 0.0)

    def to_blocks(arr):
        return arr.reshape(NUM_UTT, NUM_BLOCKS, FRAME_BLOCK, LABEL_POS).transpose(1, 0, 2, 3)

    vocab_ids = jnp.arange(VOCAB_SIZE)

    def grad_step(acc_carry, blk_in):
        gw_enc, gw_out, d_act_g = acc_carry
        enc_blk, occ_b, occ_l = blk_in
        hidden, log_probs = joint_block(enc_blk, act_g, w_enc, w_out)
        d_logits = (jnp.exp(log_probs) * (occ_b + occ_l)[..., None] - jnp.where(vocab_ids == 0, occ_b[..., None], 0.0) - jnp.where(vocab_ids == lab_ids[:, None, :, None], occ_l[..., None], 0.0)).astype(jnp.bfloat16)
        flat_dz = d_logits.reshape(NUM_UTT * FRAME_BLOCK * LABEL_POS, VOCAB_SIZE)
        flat_h = hidden.reshape(NUM_UTT * FRAME_BLOCK * LABEL_POS, JOINT_DIM)
        d_hidden = jnp.dot(flat_dz, w_out.T, preferred_element_type=jnp.float32)
        d_pre = (d_hidden * (1.0 - jnp.square(flat_h.astype(jnp.float32)))).astype(jnp.bfloat16).reshape(NUM_UTT, FRAME_BLOCK, LABEL_POS, JOINT_DIM)
        d_act_f = jnp.sum(d_pre.astype(jnp.float32), axis=2).astype(jnp.bfloat16).reshape(NUM_UTT * FRAME_BLOCK, JOINT_DIM)
        grad_blk = jnp.dot(d_act_f, w_enc.T, preferred_element_type=jnp.float32).astype(jnp.bfloat16).reshape(NUM_UTT, FRAME_BLOCK, ENC_DIM)
        gw_enc = gw_enc + jnp.dot(enc_blk.reshape(NUM_UTT * FRAME_BLOCK, ENC_DIM).T, d_act_f, preferred_element_type=jnp.float32)
        gw_out = gw_out + jnp.dot(flat_h.T, flat_dz, preferred_element_type=jnp.float32)
        d_act_g = d_act_g + jnp.sum(d_pre.astype(jnp.float32), axis=1)
        return (gw_enc, gw_out, d_act_g), grad_blk

    acc_init = (jnp.zeros((ENC_DIM, JOINT_DIM), jnp.float32), jnp.zeros((JOINT_DIM, VOCAB_SIZE), jnp.float32), jnp.zeros((NUM_UTT, LABEL_POS, JOINT_DIM), jnp.float32))
    (gw_enc, gw_out, d_act_g), grad_blocks = lax.scan(grad_step, acc_init, (enc_blocks, to_blocks(occ_blank), to_blocks(occ_lab)))
    grad_enc = grad_blocks.transpose(1, 0, 2, 3).reshape(NUM_UTT, NUM_FRAMES, ENC_DIM)
    gw_pred = jnp.einsum('buh,buj->hj', pred_out.astype(jnp.float32), d_act_g.astype(jnp.float32))
    return -log_prob, grad_enc, gw_enc, gw_pred, gw_out
```

```python
import functools

import jax
import jax.numpy as jnp
from jax import lax
from jax.experimental import pallas as pl
from jax.experimental.pallas import tpu as pltpu
from jax.sharding import PartitionSpec as P

NEG = -1.0e30
F32 = jnp.float32
BF16 = jnp.bfloat16
MESH = pl.DeviceIdType.MESH
LANES = 128
NT = (((1,), (1,)), ((), ()))
NN = (((1,), (0,)), ((), ()))
M_D, M_R1L, M_R1R, M_DL, M_DR, M_R2L, M_R2R, M_AL, M_AR, M_OA, M_OB, M_S = range(12)


def mm(a, b, dims=NN):
    return lax.dot_general(a, b, dims, preferred_element_type=F32)


def iota(shape, dim):
    return lax.broadcasted_iota(jnp.int32, shape, dim)


def lae(x, y):
    return jnp.maximum(x, y) + jnp.log(1.0 + jnp.exp(-jnp.abs(x - y)))


def kernel(n, n_utt, n_loc, n_pos,
           f_ref, g_ref, we_ref, wp_ref, wo_ref, meta_ref,
           loss_ref, gf_ref, gwe_ref, gwp_ref, gwo_ref,
           wot, at_s, ct_s, ht, e_s, dz, dhb, dad, pd,
           blank_r, lab_r, rs_r, gb_r, gl_r, sc_r,
           pm, recvp, sp, sr, sa, xb, yb,
           un, recvd, r1, dd, r2, t2, gg,
           lat_s, lat_r, snd, rcv, out_sem):
    me = lax.axis_index("seq")
    nchip = n // 2
    chip, core = me // 2, lax.rem(me, 2)
    k_r, k_l, k_o = lax.rem(chip + 1, nchip), lax.rem(chip + nchip - 1, nchip), lax.rem(chip + 2, nchip)
    right, left, sib = k_r * 2 + core, k_l * 2 + core, me + 1 - 2 * core
    hid = wo_ref.shape[0]
    voc = wo_ref.shape[1]
    enc = f_ref.shape[1]
    n_bt = n_utt * n_loc
    rows_t = n_utt * n_pos
    n_row = n_loc * rows_t

    barrier = pltpu.get_barrier_semaphore()
    for d in range(1, n):
        pl.semaphore_signal(barrier, inc=1, device_id={"seq": lax.rem(me + d, n)}, device_id_type=MESH)

    wot[...] = wo_ref[...].T
    key_r = lax.rem(iota((n_bt, 1), 0), n_loc) * n_utt + iota((n_bt, 1), 0) // n_loc
    col = iota((1, 2 * n_bt), 1)
    key_c = (col // LANES) * n_utt + lax.rem(col, n_utt)
    pd[...] = jnp.where(key_r == key_c, 1.0, 0.0).astype(BF16)
    pc = jnp.where(key_r == iota((1, rows_t), 1), 1.0, 0.0).astype(BF16)
    at = mm(we_ref[...].T, f_ref[...], NT).astype(BF16)
    at_s[...] = mm(at, pd[...])
    ct = mm(wp_ref[...].T, g_ref[...], NT).astype(BF16)
    ct_s[...] = mm(ct, pc)

    fb = rows_t // 2

    def fwd(blk, carry):
        t = blk // 2
        half = lax.rem(blk, 2)
        off = pl.multiple_of(blk * fb, fb)
        hoff = pl.multiple_of(half * fb, fb)
        a = at_s[:, pl.ds(pl.multiple_of(t * LANES, LANES), LANES)]
        c = ct_s[:, pl.ds(hoff, fb)]
        ht[:, pl.ds(off, fb)] = jnp.tanh(jnp.concatenate([a, a], axis=1) + c).astype(BF16)
        e_s[:, pl.ds(off, fb)] = mm(wot[...], ht[:, pl.ds(off, fb)])
        lab = jnp.concatenate([meta_ref[pl.ds(2 * half, 1), :], meta_ref[pl.ds(2 * half + 1, 1), :]], axis=1)
        row8 = iota((8, fb), 0)
        mx = jnp.full((8, fb), NEG, F32)
        lz = jnp.zeros((8, fb), F32)
        for i in range(voc // 8):
            z = e_s[8 * i:8 * i + 8, pl.ds(off, fb)]
            mx = jnp.maximum(mx, z)
            lz = jnp.where(row8 == lab - 8 * i, z, lz)
        z0 = e_s[0:1, pl.ds(off, fb)]
        m = jnp.max(mx, axis=0, keepdims=True)
        lz = jnp.sum(lz, axis=0, keepdims=True)
        mb = jnp.broadcast_to(m, (8, fb))
        s = jnp.zeros((8, fb), F32)
        for i in range(voc // 8):
            e = jnp.exp(e_s[8 * i:8 * i + 8, pl.ds(off, fb)] - mb)
            e_s[8 * i:8 * i + 8, pl.ds(off, fb)] = e
            s = s + e
        s = jnp.sum(s, axis=0, keepdims=True)
        lse = m + jnp.log(s)
        blank_r[pl.ds(t, 1), pl.ds(hoff, fb)] = z0 - lse
        lab_r[pl.ds(t, 1), pl.ds(hoff, fb)] = lz - lse
        rs_r[pl.ds(t, 1), pl.ds(hoff, fb)] = 1.0 / s
        return carry

    lax.fori_loop(0, n_row // fb, fwd, 0)

    lane = iota((n_loc, LANES), 1)
    low = lane < n_utt
    t_loc = iota((n_loc, LANES), 0) + me * n_loc
    t_end = jnp.broadcast_to(meta_ref[4:5, :], (n_loc, LANES))
    live = t_loc < t_end
    for u in range(n_pos):
        q = u // 2
        b = blank_r[:, LANES * q:LANES * (q + 1)]
        l = lab_r[:, LANES * q:LANES * (q + 1)]
        if u == n_pos - 1:
            l = jnp.full((n_loc, LANES), NEG, F32)
        if u % 2 == 0:
            l = pltpu.roll(l, n_utt, 1)
        else:
            b = pltpu.roll(b, n_utt, 1)
        pm[n_loc * u:n_loc * (u + 1), :] = jnp.where(low, jnp.where(live, b, 0.0), jnp.where(live, l, NEG))

    pl.semaphore_wait(barrier, n - 1)

    def lat_copy(d, dst):
        peer = lax.rem(me + d, n)
        return pltpu.make_async_remote_copy(
            src_ref=pm, dst_ref=recvp.at[me if dst else peer], send_sem=lat_s.at[d],
            recv_sem=lat_r.at[me if dst else peer], device_id={"seq": peer}, device_id_type=MESH)

    for d in range(1, n):
        lat_copy(d, True).start()

    fill_lane = iota(sp.shape, 1) < n_utt
    sp[...] = jnp.where(fill_lane, 0.0, NEG)
    sr[...] = jnp.where(fill_lane, NEG, 0.0)
    u_id = iota((n_pos, LANES), 0)
    bound = jnp.where(u_id == jnp.broadcast_to(meta_ref[5:6, :], (n_pos, LANES)), 0.0, NEG)
    init = jnp.where(u_id == 0, 0.0, NEG)

    def put(rows, src):
        for u in range(n_pos):
            x = src[n_loc * u:n_loc * (u + 1), :]
            base = rows + (n_pos + 1) * u
            sp[pl.ds(base, n_loc, stride=n_pos), :] = x
            sr[pl.ds(base, n_loc, stride=n_pos), :] = pltpu.roll(x, n_utt, 1)

    put(me * (n_loc * n_pos), pm)
    for d in range(1, n):
        peer = lax.rem(me + d, n)
        lat_copy(d, False).wait_recv()
        put(peer * (n_loc * n_pos), recvp.at[peer])

    n_diag = n * n_loc + n_pos - 1

    def lattice(step, carry):
        s_a, s_b = carry
        da = pl.multiple_of(step * n_pos, n_pos)
        db = pl.multiple_of((n_diag - 1 - step) * n_pos, n_pos)
        sa[pl.ds(da, n_pos), :] = s_a
        x_a = s_a + sp[pl.ds(da, n_pos), :]
        y_a = pltpu.roll(s_a + sr[pl.ds(da, n_pos), :], 1, 0)
        x_b = s_b + sp[pl.ds(db, n_pos), :]
        y_b = pltpu.roll(s_b, n_pos - 1, 0) + sr[pl.ds(db, n_pos), :]
        xb[pl.ds(db, n_pos), :] = x_b
        yb[pl.ds(db, n_pos), :] = y_b
        return lae(x_a, y_a), lae(x_b, y_b)

    _, s_b = lax.fori_loop(0, n_diag, lattice, (init, bound))
    logp = s_b[0:1, :]
    loss_ref[...] = jnp.broadcast_to(-logp, loss_ref.shape)
    lp8 = jnp.broadcast_to(logp, (n_loc, LANES))

    gbs, gls = [], []
    for u in range(n_pos):
        rows = pl.ds(me * (n_loc * n_pos) + (n_pos + 1) * u, n_loc, stride=n_pos)
        al = sa[rows, :] - lp8
        gbs.append(jnp.where(live, jnp.exp(jnp.minimum(al + xb[rows, :], 0.0)), 0.0))
        gls.append(jnp.where(live, jnp.exp(jnp.minimum(al + yb[rows, :], 0.0)), 0.0))
    for q in range(n_pos // 2):
        ls = slice(LANES * q, LANES * (q + 1))
        gb = jnp.where(low, gbs[2 * q], pltpu.roll(gbs[2 * q + 1], n_utt, 1))
        gl = jnp.where(low, gls[2 * q], pltpu.roll(gls[2 * q + 1], n_utt, 1))
        gb_r[:, ls] = gb
        gl_r[:, ls] = gl
        sc_r[:, ls] = (gb + gl) * rs_r[:, ls]

    u_rows = un.shape[1]
    h_rows = u_rows // 2
    p_rows = h_rows // nchip
    s_rows = p_rows // 2
    mine = core * h_rows

    def msg(kind, i, src, dst, dev):
        return pltpu.make_async_remote_copy(
            src_ref=src, dst_ref=dst, send_sem=snd.at[kind, i], recv_sem=rcv.at[kind, i],
            device_id={"seq": dev}, device_id_type=MESH)

    sent = []

    def send(*args):
        m = msg(*args)
        m.start()
        sent.append(m)

    def take(kind, i, ref):
        msg(kind, i, ref, ref, sib).wait_recv()

    def hp(i, k, lo, size):
        return un.at[i, pl.ds(mine + k * p_rows + lo, size)]

    def gp(i, k, lo, size):
        return gg.at[i, pl.ds(mine + k * p_rows + lo, size)]

    def step0(i):
        send(M_D, i, un.at[i, pl.ds((1 - core) * h_rows, h_rows)], recvd.at[i], sib)

    def step1(i):
        take(M_D, i, recvd.at[i])
        un[i, pl.ds(mine, h_rows)] += recvd[i]
        send(M_R1L, i, hp(i, k_o, 0, s_rows), r1.at[i, 0], right)
        send(M_R1R, i, hp(i, k_o, s_rows, s_rows), r1.at[i, 1], left)
        send(M_DL, i, hp(i, k_r, s_rows, s_rows), dd.at[i, 0], right)
        send(M_DR, i, hp(i, k_l, 0, s_rows), dd.at[i, 1], left)

    def step2(i):
        take(M_R1L, i, r1.at[i, 0])
        t2[i, 0] = hp(i, k_r, 0, s_rows)[...] + r1[i, 0]
        send(M_R2L, i, t2.at[i, 0], r2.at[i, 0], right)
        take(M_R1R, i, r1.at[i, 1])
        t2[i, 1] = hp(i, k_l, s_rows, s_rows)[...] + r1[i, 1]
        send(M_R2R, i, t2.at[i, 1], r2.at[i, 1], left)

    def step3(i):
        take(M_DR, i, dd.at[i, 1])
        take(M_R2L, i, r2.at[i, 0])
        gg[i, pl.ds(mine + chip * p_rows, s_rows)] = hp(i, chip, 0, s_rows)[...] + r2[i, 0] + dd[i, 1]
        take(M_DL, i, dd.at[i, 0])
        take(M_R2R, i, r2.at[i, 1])
        gg[i, pl.ds(mine + chip * p_rows + s_rows, s_rows)] = hp(i, chip, s_rows, s_rows)[...] + r2[i, 1] + dd[i, 0]
        own = gp(i, chip, 0, p_rows)
        send(M_AL, i, own, own, right)
        send(M_AR, i, own, own, left)

    def step4(i):
        take(M_AL, i, gp(i, k_l, 0, p_rows))
        send(M_OA, i, gp(i, k_l, 0, s_rows), gp(i, k_l, 0, s_rows), right)
        take(M_AR, i, gp(i, k_r, 0, p_rows))
        send(M_OB, i, gp(i, k_r, s_rows, s_rows), gp(i, k_r, s_rows, s_rows), left)

    def step5(i):
        take(M_OA, i, gp(i, k_o, 0, s_rows))
        take(M_OB, i, gp(i, k_o, s_rows, s_rows))
        half = gg.at[i, pl.ds(mine, h_rows)]
        send(M_S, i, half, half, sib)

    outs = []

    def step6(i):
        take(M_S, i, gg.at[i, pl.ds((1 - core) * h_rows, h_rows)])
        if i < 4:
            for s in range(2):
                cols = slice((2 * i + s) * LANES, (2 * i + s + 1) * LANES)
                cp = pltpu.make_async_copy(gg.at[i, pl.ds(s * hid, hid)], gwo_ref.at[:, cols], out_sem.at[i, s])
                cp.start()
                outs.append(cp)
        elif i == 7:
            n_blk = hid // LANES
            for s in range(n_blk):
                cols = slice(s * LANES, (s + 1) * LANES)
                lo, hi = s * enc, (s + 1) * enc
                first = lo
                while first < hi:
                    unit = first // u_rows
                    last = min(hi, (unit + 1) * u_rows)
                    cp = pltpu.make_async_copy(
                        gg.at[6 + unit, pl.ds(first - unit * u_rows, last - first)],
                        gwe_ref.at[pl.ds(first - lo, last - first), cols], out_sem.at[4 + unit, s])
                    cp.start()
                    outs.append(cp)
                    first = last

    steps = (step0, step1, step2, step3, step4, step5, step6)
    done = [0] * 8

    def advance(*units):
        for i in units:
            steps[done[i]](i)
            done[i] += 1

    vb = u_rows // hid * LANES

    def make_dz(i):
        def per_t(t, carry):
            off = pl.multiple_of(t * rows_t, rows_t)
            sc = sc_r[pl.ds(t, 1), :]
            gl = gl_r[pl.ds(t, 1), :]
            lab = jnp.concatenate([meta_ref[q:q + 1, :] for q in range(4)], axis=1)
            scb = jnp.broadcast_to(sc, (16, rows_t))
            glb = jnp.broadcast_to(gl, (16, rows_t))
            row = iota((16, rows_t), 0)

            def grp(j, c2):
                r0 = pl.multiple_of(i * vb + j * 16, 16)
                x = e_s[pl.ds(r0, 16), pl.ds(off, rows_t)] * scb
                x = jnp.where(row == lab - r0, x - glb, x)
                dz[pl.ds(r0, 16), pl.ds(off, rows_t)] = x.astype(BF16)
                return c2

            lax.fori_loop(0, vb // 16, grp, 0)
            if i == 0:
                gb = gb_r[pl.ds(t, 1), :]
                x = e_s[0:16, pl.ds(off, rows_t)] * scb
                x = jnp.where(row == lab, x - glb, x)
                x = jnp.where(row == 0, x - jnp.broadcast_to(gb, (16, rows_t)), x)
                dz[0:16, pl.ds(off, rows_t)] = x.astype(BF16)
            return carry

        lax.fori_loop(0, n_loc, per_t, 0)

    def make_out(i):
        un[i] = jnp.zeros((u_rows, LANES), F32)
        kc = n_row // 4

        def chunk(r, carry):
            lo = pl.multiple_of(r * kc, kc)
            x = mm(ht[:, pl.ds(lo, kc)], dz[i * vb:(i + 1) * vb, pl.ds(lo, kc)], NT)
            un[i, 0:hid] += x[:, 0:LANES]
            un[i, hid:2 * hid] += x[:, LANES:2 * LANES]
            return carry

        lax.fori_loop(0, 4, chunk, 0)

    for i in range(4):
        make_dz(i)
        make_out(i)
        advance(i)
        for j in range(i - 1, -1, -1):
            advance(j)

    un[4:6] = jnp.zeros((2, u_rows, LANES), F32)

    def back(t, carry):
        off = pl.multiple_of(t * rows_t, rows_t)
        dhb[...] = mm(wo_ref[...], dz[:, pl.ds(off, rows_t)])
        for i in range(hid // 16):
            rr = slice(16 * i, 16 * i + 16)
            h = ht[rr, pl.ds(off, rows_t)].astype(F32)
            dp = (dhb[rr, :] * (1.0 - h * h)).astype(BF16).astype(F32)
            x = None
            for q in range(rows_t // LANES):
                y = dp[:, q * LANES:(q + 1) * LANES]
                lo = q % 2 * hid + 16 * i
                un[4 + q // 2, lo:lo + 16] += y
                x = y if x is None else x + y
            x = x + pltpu.roll(x, n_utt, 1)
            x = jnp.where(iota((16, LANES), 1) < n_utt, x, 0.0)
            dad[rr, pl.ds(pl.multiple_of(t * LANES, LANES), LANES)] = x.astype(BF16)
        return carry

    for part in range(4):
        lax.fori_loop(part * n_loc // 4, (part + 1) * n_loc // 4, back, 0)
        for j in range(4):
            if done[j] < 7:
                advance(j)

    for i in range(2):
        advance(4 + i)
    da = mm(pd[...], dad[...], NT).astype(BF16)
    advance(4, 5)
    x = mm(f_ref[...].T, da)
    for s in range(hid // LANES):
        lo, hi = s * enc, (s + 1) * enc
        first = lo
        while first < hi:
            unit = first // u_rows
            last = min(hi, (unit + 1) * u_rows)
            un[6 + unit, first - unit * u_rows:last - unit * u_rows] = x[first - lo:last - lo, s * LANES:(s + 1) * LANES]
            first = last
    advance(6, 7)
    gf_ref[...] = mm(da, we_ref[...], NT).astype(BF16)
    gpt = mm(g_ref[...].T, pc).astype(BF16)
    while min(done) < 7:
        order = sorted(range(8), key=lambda j: (-done[j], j))
        for j in order:
            if done[j] < 7:
                advance(j)
    dcb = jnp.concatenate([gg[4, 0:hid], gg[4, hid:2 * hid], gg[5, 0:hid], gg[5, hid:2 * hid]], axis=1).astype(BF16)
    gwp_ref[...] = mm(gpt, dcb, NT)
    for m in sent:
        m.wait_send()
    for d in range(1, n):
        lat_copy(d, True).wait_send()
    for cp in outs:
        cp.wait()


def solution(mesh):
    n = mesh.shape["seq"]

    def local_fn(enc_out, pred_out, w_enc, w_pred, w_out, labels, frame_len, label_len):
        n_utt, n_loc, enc = enc_out.shape
        n_pos, pred = pred_out.shape[1:]
        hid, voc = w_out.shape
        assert n == 8 and 2 * n_utt == LANES and n_loc == 8 and n_pos == 8
        n_bt = n_utt * n_loc
        rows_t = n_utt * n_pos
        n_row = n_loc * rows_t
        lab = jnp.concatenate([labels.T, jnp.full((1, n_utt), -1, jnp.int32)], axis=0).reshape(n_pos // 2, LANES)
        lens = jnp.stack([frame_len, label_len])
        lens = jnp.concatenate([lens, lens], axis=1)
        meta = jnp.concatenate([lab, lens, jnp.zeros((2, LANES), jnp.int32)], axis=0)
        u_rows = 2 * hid
        h_rows = u_rows // 2
        s_rows = h_rows // n
        vm = pl.BlockSpec(memory_space=pltpu.VMEM)
        anys = pl.BlockSpec(memory_space=pl.ANY)
        n_sk = (n * n_loc + n_pos) * n_pos
        scratch = [
            pltpu.VMEM((voc, hid), BF16),
            pltpu.VMEM((hid, n_loc * LANES), F32),
            pltpu.VMEM((hid, rows_t), F32),
            pltpu.VMEM((hid, n_row), BF16),
            pltpu.VMEM((voc, n_row), F32),
            pltpu.VMEM((voc, n_row), BF16),
            pltpu.VMEM((hid, rows_t), F32),
            pltpu.VMEM((hid, n_loc * LANES), BF16),
            pltpu.VMEM((n_bt, n_loc * LANES), BF16),
        ] + [pltpu.VMEM((n_loc, rows_t), F32)] * 6 + [
            pltpu.VMEM((n_loc * n_pos, LANES), F32),
            pltpu.VMEM((n, n_loc * n_pos, LANES), F32),
        ] + [pltpu.VMEM((n_sk, LANES), F32)] * 5 + [
            pltpu.VMEM((8, u_rows, LANES), F32),
            pltpu.VMEM((8, h_rows, LANES), F32),
            pltpu.VMEM((8, 2, s_rows, LANES), F32),
            pltpu.VMEM((8, 2, s_rows, LANES), F32),
            pltpu.VMEM((8, 2, s_rows, LANES), F32),
            pltpu.VMEM((8, 2, s_rows, LANES), F32),
            pltpu.VMEM((8, u_rows, LANES), F32),
            pltpu.SemaphoreType.DMA((n,)),
            pltpu.SemaphoreType.DMA((n,)),
            pltpu.SemaphoreType.DMA((12, 8)),
            pltpu.SemaphoreType.DMA((12, 8)),
            pltpu.SemaphoreType.DMA((6, 5)),
        ]
        loss, gf, gwe, gwp, gwo = pl.pallas_call(
            functools.partial(kernel, n, n_utt, n_loc, n_pos),
            out_shape=(
                jax.ShapeDtypeStruct((8, LANES), F32),
                jax.ShapeDtypeStruct((n_bt, enc), BF16),
                jax.ShapeDtypeStruct((enc, hid), F32),
                jax.ShapeDtypeStruct((pred, hid), F32),
                jax.ShapeDtypeStruct((hid, voc), F32),
            ),
            in_specs=[vm] * 6,
            out_specs=(vm, vm, anys, vm, anys),
            scratch_shapes=scratch,
            compiler_params=pltpu.CompilerParams(collective_id=0, has_side_effects=True, vmem_limit_bytes=67043328),
            name="rnnt",
        )(enc_out.reshape(n_bt, enc), pred_out.reshape(n_utt * n_pos, pred), w_enc, w_pred, w_out, meta)
        return loss[0, :n_utt], gf.reshape(n_utt, n_loc, enc), gwe, gwp, gwo

    in_specs = (P("dp", "seq", None), P("dp", None, None), P(None, None), P(None, None), P(None, None), P("dp", None), P("dp"), P("dp"))
    out_specs = (P("dp"), P("dp", "seq", None), P("dp", None), P("dp", None), P("dp", None))
    return jax.shard_map(local_fn, mesh=mesh, in_specs=in_specs, out_specs=out_specs, check_vma=False)
```

```python
import functools

import jax
import jax.numpy as jnp
from jax import lax
from jax.experimental import pallas as pl
from jax.experimental.pallas import tpu as pltpu
from jax.sharding import PartitionSpec as P

NEG = -1.0e30
F32 = jnp.float32
BF16 = jnp.bfloat16
MESH = pl.DeviceIdType.MESH
LANES = 128
VMEM_LIMIT = 57 * 2 ** 20
NT = (((1,), (1,)), ((), ()))
NN = (((1,), (0,)), ((), ()))
M_D, M_R1L, M_R1R, M_DL, M_DR, M_R2L, M_R2R, M_AL, M_AR, M_OA, M_OB, M_S = range(12)


def mm(a, b, dims=NN):
    return lax.dot_general(a, b, dims, preferred_element_type=F32)


def iota(shape, dim):
    return lax.broadcasted_iota(jnp.int32, shape, dim)


def lae(x, y):
    return jnp.maximum(x, y) + jnp.log(1.0 + jnp.exp(-jnp.abs(x - y)))


LINK_RATE, LINK_LAT, CORE_RATE, CORE_LAT = 46.6e3, 1.9, 600e3, 1.1
NEEDS = ((), (M_D,), (M_R1L, M_R1R), (M_DL, M_DR, M_R2L, M_R2R), (M_AL, M_AR), (M_OA, M_OB), (M_S,))
COSTS = (.02, .25, .1, .2, .05, .05, .05)


def static_order(segs, piece, narrow):
    now, free, arrive, done, order, made = 0.0, {}, {}, {}, [], []

    def tx(kind, u, link, size):
        rate, lat = (CORE_RATE, CORE_LAT) if link == "c" else (LINK_RATE, LINK_LAT)
        begin = max(now, free.get(link, 0.0))
        free[link] = begin + size / rate
        arrive[kind, u] = free[link] + lat

    def ready(u):
        return max([arrive[k, u] for k in NEEDS[done[u]]], default=0.0)

    def step(u):
        nonlocal now
        k = done[u]
        now = max(now, ready(u)) + COSTS[k]
        ag = piece / 2 if u in narrow else piece
        if k == 0:
            tx(M_D, u, "c", 4 * piece)
        elif k == 1:
            for kind, link in ((M_R1L, "r"), (M_R1R, "l"), (M_DL, "r"), (M_DR, "l")):
                tx(kind, u, link, piece / 2)
        elif k == 2:
            tx(M_R2L, u, "r", piece / 2)
            tx(M_R2R, u, "l", piece / 2)
        elif k == 3:
            tx(M_AL, u, "r", ag)
            tx(M_AR, u, "l", ag)
        elif k == 4:
            tx(M_OA, u, "r", ag / 2)
            tx(M_OB, u, "l", ag / 2)
        elif k == 5:
            tx(M_S, u, "c", 4 * ag)
        done[u] += 1
        order.append((1, u))

    left = list(range(len(segs)))
    while True:
        cand = [u for u in made if done[u] < 7]
        now_ready = [u for u in cand if ready(u) <= now]
        if now_ready:
            step(min(now_ready, key=lambda u: (done[u] > 3, made.index(u))))
        elif left:
            i = left.pop(0)
            order.append((0, i))
            now += segs[i][0]
            for u in segs[i][2]:
                made.append(u)
                done[u] = 0
        elif cand:
            step(min(cand, key=ready))
        else:
            return order


def kernel(n, n_utt, n_loc, n_pos,
           f_ref, g_ref, we_ref, wp_ref, wo_ref, lab_ref, flen_ref, llen_ref,
           loss_ref, gf_ref, gg, gd, gpt_ref,
           wot, at_s, ct_s, ht, e_s, za, zc, dz0, dz1, dz2, dz3, dad, dacc, pd, trs, lab_s, len_s,
           blank_r, lab_r, rs_r, gb_r, gl_r, sc_r,
           pm, recvp, sp, sr, sa, xb, yb,
           un, recvd, r1, dd, r2, t2,
           lat_s, lat_r, snd, rcv):
    me = lax.axis_index("seq")
    nchip = n // 2
    chip, core = me // 2, lax.rem(me, 2)
    k_r, k_l, k_o = lax.rem(chip + 1, nchip), lax.rem(chip + nchip - 1, nchip), lax.rem(chip + 2, nchip)
    right, left, sib = k_r * 2 + core, k_l * 2 + core, me + 1 - 2 * core
    hid = wo_ref.shape[0]
    voc = wo_ref.shape[1]
    enc = f_ref.shape[1]
    n_bt = n_utt * n_loc
    rows_t = n_utt * n_pos
    n_row = n_loc * rows_t

    barrier = pltpu.get_barrier_semaphore()
    for d in range(1, n):
        pl.semaphore_signal(barrier, inc=1, device_id={"seq": lax.rem(me + d, n)}, device_id_type=MESH)

    wot[...] = wo_ref[...].T
    trs[...] = jnp.full(trs.shape, -1, jnp.int32)
    trs[0:n_pos - 1, 0:n_utt] = lab_ref[...]
    lab_t = trs[...]
    lab_alt = pltpu.roll(lab_t, n_utt, 1)
    low1 = iota((1, LANES), 1) < n_utt
    for q in range(n_pos // 2):
        lab_s[0:1, LANES * q:LANES * (q + 1)] = jnp.where(low1, lab_t[2 * q:2 * q + 1], lab_alt[2 * q + 1:2 * q + 2])
    len_s[0:1, 0:n_utt] = flen_ref[...]
    len_s[1:2, 0:n_utt] = llen_ref[...]
    key_r = lax.rem(iota((n_bt, 1), 0), n_loc) * n_utt + iota((n_bt, 1), 0) // n_loc
    col = iota((1, 2 * n_bt), 1)
    key_c = (col // LANES) * n_utt + lax.rem(col, n_utt)
    pd[...] = jnp.where(key_r == key_c, 1.0, 0.0).astype(BF16)
    pc = jnp.where(key_r == iota((1, rows_t), 1), 1.0, 0.0).astype(BF16)
    at = mm(we_ref[...].T, f_ref[...], NT).astype(BF16)
    at_s[...] = mm(at, pd[...]).astype(BF16)
    ct = mm(wp_ref[...].T, g_ref[...], NT).astype(BF16)
    ct_s[...] = mm(ct, pc).astype(BF16)
    gpt_ref[...] = mm(g_ref[...].T, pc).astype(BF16)

    fb = rows_t // 2
    n_blk = n_row // fb

    def logits(blk, z_ref):
        t = blk // 2
        off = pl.multiple_of(blk * fb, fb)
        a = at_s[:, pl.ds(pl.multiple_of(t * LANES, LANES), LANES)].astype(F32)
        c = ct_s[:, pl.ds(pl.multiple_of(lax.rem(blk, 2) * fb, fb), fb)].astype(F32)
        h = jnp.tanh(jnp.concatenate([a, a], axis=1) + c).astype(BF16)
        ht[:, pl.ds(off, fb)] = h
        z_ref[...] = mm(wot[...], h)

    def norm(blk, z_ref):
        t = blk // 2
        off = pl.multiple_of(blk * fb, fb)
        hoff = pl.multiple_of(lax.rem(blk, 2) * fb, fb)
        lab = lab_s[0:1, pl.ds(hoff, fb)]
        ch = LANES
        row = iota((ch, fb), 0)
        mx = jnp.full((8, fb), NEG, F32)
        lz = jnp.zeros((8, fb), F32)
        for i in range(voc // ch):
            z = z_ref[ch * i:ch * (i + 1), :]
            hit = jnp.where(row == lab - ch * i, z, 0.0)
            mx = jnp.maximum(mx, jnp.max(z.reshape(ch // 8, 8, fb), axis=0))
            lz = lz + jnp.sum(hit.reshape(ch // 8, 8, fb), axis=0)
        m = jnp.max(mx, axis=0, keepdims=True)
        lz = jnp.sum(lz, axis=0, keepdims=True)
        s = jnp.zeros((8, fb), F32)
        for i in range(voc // ch):
            e = jnp.exp(z_ref[ch * i:ch * (i + 1), :] - m)
            e_s[ch * i:ch * (i + 1), pl.ds(off, fb)] = e
            s = s + jnp.sum(e.reshape(ch // 8, 8, fb), axis=0)
        s = jnp.sum(s, axis=0, keepdims=True)
        lse = m + jnp.log(s)
        blank_r[pl.ds(t, 1), pl.ds(hoff, fb)] = z_ref[0:1, :] - lse
        lab_r[pl.ds(t, 1), pl.ds(hoff, fb)] = lz - lse
        rs_r[pl.ds(t, 1), pl.ds(hoff, fb)] = 1.0 / s

    def fwd(j, carry):
        logits(2 * j + 1, zc)
        norm(2 * j, za)
        logits(2 * j + 2, za)
        norm(2 * j + 1, zc)
        return carry

    logits(0, za)
    lax.fori_loop(0, n_blk // 2 - 1, fwd, 0)
    logits(n_blk - 1, zc)
    norm(n_blk - 2, za)
    norm(n_blk - 1, zc)

    lane = iota((n_loc, LANES), 1)
    low = lane < n_utt
    t_loc = iota((n_loc, LANES), 0) + me * n_loc
    len2 = jnp.where(low1, len_s[0:1, :], pltpu.roll(len_s[0:1, :], n_utt, 1))
    t_end = jnp.broadcast_to(len2, (n_loc, LANES))
    live = t_loc < t_end
    for u in range(n_pos):
        q = u // 2
        b = blank_r[:, LANES * q:LANES * (q + 1)]
        l = lab_r[:, LANES * q:LANES * (q + 1)]
        if u == n_pos - 1:
            l = jnp.full((n_loc, LANES), NEG, F32)
        if u % 2 == 0:
            l = pltpu.roll(l, n_utt, 1)
        else:
            b = pltpu.roll(b, n_utt, 1)
        pm[n_loc * u:n_loc * (u + 1), :] = jnp.where(low, jnp.where(live, b, 0.0), jnp.where(live, l, NEG))

    pl.semaphore_wait(barrier, n - 1)

    def lat_copy(d, dst):
        peer = lax.rem(me + d, n)
        return pltpu.make_async_remote_copy(
            src_ref=pm, dst_ref=recvp.at[me if dst else peer], send_sem=lat_s.at[d],
            recv_sem=lat_r.at[me if dst else peer], device_id={"seq": peer}, device_id_type=MESH)

    for d in range(1, n):
        lat_copy(d, True).start()

    fill_lane = iota(sp.shape, 1) < n_utt
    sp[...] = jnp.where(fill_lane, 0.0, NEG)
    sr[...] = jnp.where(fill_lane, NEG, 0.0)
    u_id = iota((n_pos, LANES), 0)
    bound = jnp.where(u_id == jnp.broadcast_to(len_s[1:2, :], (n_pos, LANES)), 0.0, NEG)
    init = jnp.where(u_id == 0, 0.0, NEG)

    def put(rows, src):
        for u in range(n_pos):
            x = src[n_loc * u:n_loc * (u + 1), :]
            base = rows + (n_pos + 1) * u
            sp[pl.ds(base, n_loc, stride=n_pos), :] = x
            sr[pl.ds(base, n_loc, stride=n_pos), :] = pltpu.roll(x, n_utt, 1)

    put(me * (n_loc * n_pos), pm)
    for d in range(1, n):
        peer = lax.rem(me + d, n)
        lat_copy(d, False).wait_recv()
        put(peer * (n_loc * n_pos), recvp.at[peer])

    n_diag = n * n_loc + n_pos - 1

    def lattice(step, carry):
        s_a, s_b = carry
        da = pl.multiple_of(step * n_pos, n_pos)
        db = pl.multiple_of((n_diag - 1 - step) * n_pos, n_pos)
        sa[pl.ds(da, n_pos), :] = s_a
        x_a = s_a + sp[pl.ds(da, n_pos), :]
        y_a = pltpu.roll(s_a + sr[pl.ds(da, n_pos), :], 1, 0)
        x_b = s_b + sp[pl.ds(db, n_pos), :]
        y_b = pltpu.roll(s_b, n_pos - 1, 0) + sr[pl.ds(db, n_pos), :]
        xb[pl.ds(db, n_pos), :] = x_b
        yb[pl.ds(db, n_pos), :] = y_b
        return lae(x_a, y_a), lae(x_b, y_b)

    _, s_b = lax.fori_loop(0, n_diag, lattice, (init, bound))
    logp = s_b[0:1, :]
    loss_ref[...] = jnp.broadcast_to(-logp, loss_ref.shape)
    lp8 = jnp.broadcast_to(logp, (n_loc, LANES))

    gbs, gls = [], []
    for u in range(n_pos):
        rows = pl.ds(me * (n_loc * n_pos) + (n_pos + 1) * u, n_loc, stride=n_pos)
        al = sa[rows, :] - lp8
        gbs.append(jnp.where(live, jnp.exp(jnp.minimum(al + xb[rows, :], 0.0)), 0.0))
        gls.append(jnp.where(live, jnp.exp(jnp.minimum(al + yb[rows, :], 0.0)), 0.0))
    for q in range(n_pos // 2):
        ls = slice(LANES * q, LANES * (q + 1))
        gb = jnp.where(low, gbs[2 * q], pltpu.roll(gbs[2 * q + 1], n_utt, 1))
        gl = jnp.where(low, gls[2 * q], pltpu.roll(gls[2 * q + 1], n_utt, 1))
        gb_r[:, ls] = gb
        gl_r[:, ls] = gl
        sc_r[:, ls] = (gb + gl) * rs_r[:, ls]

    u_rows = un.shape[1]
    h_rows = u_rows // 2
    p_rows = h_rows // nchip
    s_rows = p_rows // 2
    mine = core * h_rows

    def msg(kind, i, src, dst, dev):
        return pltpu.make_async_remote_copy(
            src_ref=src, dst_ref=dst, send_sem=snd.at[kind, i], recv_sem=rcv.at[kind, i],
            device_id={"seq": dev}, device_id_type=MESH)

    sent = []

    def send(*args):
        m = msg(*args)
        m.start()
        sent.append(m)

    def take(kind, i, ref):
        msg(kind, i, ref, ref, sib).wait_recv()

    def hp(i, k, lo, size):
        return un.at[i, pl.ds(mine + k * p_rows + lo, size)]

    narrow = (6, 7)

    def final(i, lo, size):
        return (gd.at[i - 6] if i in narrow else gg.at[i]).at[pl.ds(lo, size)]

    def gp(i, k, lo, size):
        return final(i, mine + k * p_rows + lo, size)

    def step0(i):
        send(M_D, i, un.at[i, pl.ds((1 - core) * h_rows, h_rows)], recvd.at[i], sib)

    def step1(i):
        take(M_D, i, recvd.at[i])
        un[i, pl.ds(mine, h_rows)] += recvd[i]
        send(M_R1L, i, hp(i, k_o, 0, s_rows), r1.at[i, 0], right)
        send(M_R1R, i, hp(i, k_o, s_rows, s_rows), r1.at[i, 1], left)
        send(M_DL, i, hp(i, k_r, s_rows, s_rows), dd.at[i, 0], right)
        send(M_DR, i, hp(i, k_l, 0, s_rows), dd.at[i, 1], left)

    def step2(i):
        take(M_R1L, i, r1.at[i, 0])
        t2[i, 0] = hp(i, k_r, 0, s_rows)[...] + r1[i, 0]
        send(M_R2L, i, t2.at[i, 0], r2.at[i, 0], right)
        take(M_R1R, i, r1.at[i, 1])
        t2[i, 1] = hp(i, k_l, s_rows, s_rows)[...] + r1[i, 1]
        send(M_R2R, i, t2.at[i, 1], r2.at[i, 1], left)

    def step3(i):
        take(M_DR, i, dd.at[i, 1])
        take(M_R2L, i, r2.at[i, 0])
        res, lo = (gd, i - 6) if i in narrow else (gg, i)
        res[lo, pl.ds(mine + chip * p_rows, s_rows)] = (hp(i, chip, 0, s_rows)[...] + r2[i, 0] + dd[i, 1]).astype(res.dtype)
        take(M_DL, i, dd.at[i, 0])
        take(M_R2R, i, r2.at[i, 1])
        res[lo, pl.ds(mine + chip * p_rows + s_rows, s_rows)] = (hp(i, chip, s_rows, s_rows)[...] + r2[i, 1] + dd[i, 0]).astype(res.dtype)
        own = gp(i, chip, 0, p_rows)
        send(M_AL, i, own, own, right)
        send(M_AR, i, own, own, left)

    def step4(i):
        take(M_AL, i, gp(i, k_l, 0, p_rows))
        send(M_OA, i, gp(i, k_l, 0, s_rows), gp(i, k_l, 0, s_rows), right)
        take(M_AR, i, gp(i, k_r, 0, p_rows))
        send(M_OB, i, gp(i, k_r, s_rows, s_rows), gp(i, k_r, s_rows, s_rows), left)

    def step5(i):
        take(M_OA, i, gp(i, k_o, 0, s_rows))
        take(M_OB, i, gp(i, k_o, s_rows, s_rows))
        half = final(i, mine, h_rows)
        send(M_S, i, half, half, sib)

    def step6(i):
        take(M_S, i, final(i, (1 - core) * h_rows, h_rows))

    steps = (step0, step1, step2, step3, step4, step5, step6)
    done = [0] * 8

    def advance(*units):
        for i in units:
            steps[done[i]](i)
            done[i] += 1

    vb = u_rows // hid * LANES
    dzs = (dz0, dz1, dz2, dz3)
    kc = n_row // 4

    dc = 32

    def dz_t(i, t):
        off = pl.multiple_of(t * rows_t, rows_t)
        cols = pl.ds(off, rows_t)
        sc = sc_r[pl.ds(t, 1), :]
        gl = gl_r[pl.ds(t, 1), :]
        row = iota((dc, rows_t), 0)
        for j in range(vb // dc):
            r0 = i * vb + dc * j
            x = e_s[r0:r0 + dc, cols] * sc
            x = jnp.where(row == lab_s[0:1, :] - r0, x - gl, x)
            if r0 == 0:
                x = jnp.where(row == 0, x - gb_r[pl.ds(t, 1), :], x)
            dzs[i][dc * j:dc * (j + 1), cols] = x.astype(BF16)

    def first_dz():
        def body(t, carry):
            dz_t(0, t)
            return carry
        lax.fori_loop(0, n_loc, body, 0)

    def out_part(i, part):
        def body(r, carry):
            lo = pl.multiple_of(r * kc, kc)
            x = mm(ht[:, pl.ds(lo, kc)], dzs[i][:, pl.ds(lo, kc)], NT)
            for s in range(2):
                y = x[:, s * LANES:(s + 1) * LANES]
                if part == 0:
                    y = y + jnp.where(r == 0, 0.0, un[i, s * hid:(s + 1) * hid])
                else:
                    y = y + un[i, s * hid:(s + 1) * hid]
                un[i, s * hid:(s + 1) * hid] = y
            if i < 3:
                dz_t(i + 1, 2 * r)
                dz_t(i + 1, 2 * r + 1)
            return carry
        lax.fori_loop(2 * part, 2 * part + 2, body, 0)

    def dh(blk, z_ref):
        cols = pl.ds(pl.multiple_of(blk * fb, fb), fb)
        x = mm(wo_ref[:, 0:vb], dz0[:, cols])
        for i in range(1, 4):
            x = x + mm(wo_ref[:, i * vb:(i + 1) * vb], dzs[i][:, cols])
        z_ref[0:hid, :] = x

    dr = 64

    def dp(t, half, z_ref):
        cols = pl.ds(pl.multiple_of(t * rows_t + half * fb, fb), fb)
        low = iota((dr, LANES), 1) < n_utt
        for i in range(hid // dr):
            rr = slice(dr * i, dr * (i + 1))
            h = ht[rr, cols].astype(F32)
            x = (z_ref[rr, :] * (1.0 - h * h)).astype(BF16).astype(F32)
            x0, x1 = x[:, 0:LANES], x[:, LANES:2 * LANES]
            un[6 + half, rr, :] += x0
            un[6 + half, hid + dr * i:hid + dr * (i + 1), :] += x1
            if half == 0:
                dacc[rr, :] = x0 + x1
            else:
                acc = x0 + x1 + dacc[rr, :]
                acc = acc + pltpu.roll(acc, n_utt, 1)
                dad[rr, pl.ds(pl.multiple_of(t * LANES, LANES), LANES)] = jnp.where(low, acc, 0.0).astype(BF16)

    n_back = 4

    def back(part):
        if part == 0:
            un[6:8] = jnp.zeros((2, u_rows, LANES), F32)
            dh(0, za)

        def body(t, carry):
            dh(2 * t + 1, zc)
            dp(t, 0, za)
            dh(jnp.minimum(2 * t + 2, n_blk - 1), za)
            dp(t, 1, zc)
            return carry

        lax.fori_loop(part * n_loc // n_back, (part + 1) * n_loc // n_back, body, 0)

    def grad_w_enc():
        da = mm(pd[...], dad[...], NT).astype(BF16)
        gf_ref[...] = mm(da, we_ref[...], NT).astype(BF16)
        x = mm(f_ref[...].T, da)
        for s in range(hid // LANES):
            lo, hi = s * enc, (s + 1) * enc
            first = lo
            while first < hi:
                unit = first // u_rows
                last = min(hi, (unit + 1) * u_rows)
                un[4 + unit, first - unit * u_rows:last - unit * u_rows] = x[first - lo:last - lo, s * LANES:(s + 1) * LANES]
                first = last

    segs = [(1.5, first_dz, ())]
    for i in range(4):
        for part in range(2):
            segs.append((.85, functools.partial(out_part, i, part), (i,) if part == 1 else ()))
    for part in range(n_back):
        segs.append((2.0, functools.partial(back, part), (6, 7) if part == n_back - 1 else ()))
    segs.append((2.0, grad_w_enc, (4, 5)))
    for what, i in static_order(segs, p_rows * LANES * 4, narrow):
        if what:
            advance(i)
        else:
            segs[i][1]()
    for m in sent:
        m.wait_send()
    for d in range(1, n):
        lat_copy(d, True).wait_send()


def finish(n_utt, enc, loss_in, gf_in, gg, gd, gpt, loss_ref, gf_ref, gwe_ref, gwp_ref, gwo_ref, sem):
    hid = gpt.shape[0]
    u_rows = gg.shape[1]
    copies = []

    def copy(src, dst):
        cp = pltpu.make_async_copy(src, dst, sem.at[len(copies)])
        cp.start()
        copies.append(cp)

    for i in range(4):
        for s in range(2):
            lo = (2 * i + s) * LANES
            copy(gg.at[i, pl.ds(s * hid, hid)], gwo_ref.at[:, pl.ds(lo, LANES)])
    copy(gf_in, gf_ref)
    for s in range(hid // LANES):
        lo, hi = s * enc, (s + 1) * enc
        first = lo
        while first < hi:
            unit = first // u_rows
            last = min(hi, (unit + 1) * u_rows)
            copy(gg.at[4 + unit, pl.ds(first - unit * u_rows, last - first)],
                 gwe_ref.at[pl.ds(first - lo, last - first), pl.ds(s * LANES, LANES)])
            first = last
    loss_ref[...] = loss_in[0:1, 0:n_utt].reshape(n_utt)
    dcb = jnp.concatenate([gd[0, 0:hid], gd[0, hid:2 * hid], gd[1, 0:hid], gd[1, hid:2 * hid]], axis=1)
    gwp_ref[...] = mm(gpt[...], dcb, NT)
    for cp in copies:
        cp.wait()


def solution(mesh):
    n = mesh.shape["seq"]

    def local_fn(enc_out, pred_out, w_enc, w_pred, w_out, labels, frame_len, label_len):
        n_utt, n_loc, enc = enc_out.shape
        n_pos, pred = pred_out.shape[1:]
        hid, voc = w_out.shape
        assert n == 8 and 2 * n_utt == LANES and n_loc == 8 and n_pos == 8
        n_bt = n_utt * n_loc
        rows_t = n_utt * n_pos
        n_row = n_loc * rows_t
        u_rows = 2 * hid
        h_rows = u_rows // 2
        s_rows = h_rows // n
        vm = pl.BlockSpec(memory_space=pltpu.VMEM)
        anys = pl.BlockSpec(memory_space=pl.ANY)
        n_sk = (n * n_loc + n_pos) * n_pos
        vmem = pltpu.VMEM
        scratch = [
            vmem((voc, hid), BF16),
            vmem((hid, n_loc * LANES), BF16),
            vmem((hid, rows_t), BF16),
            vmem((hid, n_row), BF16),
            vmem((voc, n_row), F32),
            vmem((voc, rows_t // 2), F32),
            vmem((voc, rows_t // 2), F32),
        ] + [vmem((voc // 4, n_row), BF16)] * 4 + [
            vmem((hid, n_loc * LANES), BF16),
            vmem((hid, LANES), F32),
            vmem((n_bt, n_loc * LANES), BF16),
            vmem((n_pos, LANES), jnp.int32),
            vmem((8, rows_t), jnp.int32),
            vmem((8, LANES), jnp.int32),
        ] + [vmem((n_loc, rows_t), F32)] * 6 + [
            vmem((n_loc * n_pos, LANES), F32),
            vmem((n, n_loc * n_pos, LANES), F32),
        ] + [vmem((n_sk, LANES), F32)] * 5 + [
            vmem((8, u_rows, LANES), F32),
            vmem((8, h_rows, LANES), F32),
        ] + [vmem((8, 2, s_rows, LANES), F32)] * 4 + [
            pltpu.SemaphoreType.DMA((n,)),
            pltpu.SemaphoreType.DMA((n,)),
            pltpu.SemaphoreType.DMA((12, 8)),
            pltpu.SemaphoreType.DMA((12, 8)),
        ]
        mid = pl.pallas_call(
            functools.partial(kernel, n, n_utt, n_loc, n_pos),
            out_shape=(
                vmem((8, LANES), F32),
                vmem((n_bt, enc), BF16),
                vmem((6, u_rows, LANES), F32),
                vmem((2, u_rows, LANES), BF16),
                vmem((hid, rows_t), BF16),
            ),
            in_specs=[vm] * 8,
            out_specs=(vm,) * 5,
            scratch_shapes=scratch,
            compiler_params=pltpu.CompilerParams(collective_id=0, has_side_effects=True, vmem_limit_bytes=VMEM_LIMIT),
            name="rnnt",
        )(enc_out.reshape(n_bt, enc), pred_out.reshape(n_utt * n_pos, pred), w_enc, w_pred, w_out, labels.T, frame_len.reshape(1, n_utt), label_len.reshape(1, n_utt))
        mid = [pltpu.with_memory_space_constraint(x, pltpu.VMEM) for x in mid]
        loss, gf, gwe, gwp, gwo = pl.pallas_call(
            functools.partial(finish, n_utt, enc),
            out_shape=(
                jax.ShapeDtypeStruct((n_utt,), F32),
                jax.ShapeDtypeStruct((n_bt, enc), BF16),
                jax.ShapeDtypeStruct((enc, hid), F32),
                jax.ShapeDtypeStruct((pred, hid), F32),
                jax.ShapeDtypeStruct((hid, voc), F32),
            ),
            in_specs=[vm] * 5,
            out_specs=(vm, anys, anys, vm, anys),
            scratch_shapes=[pltpu.SemaphoreType.DMA((24,))],
            compiler_params=pltpu.CompilerParams(vmem_limit_bytes=8 * 2 ** 20),
            name="finish",
        )(*mid)
        return loss, gf.reshape(n_utt, n_loc, enc), gwe, gwp, gwo

    in_specs = (P("dp", "seq", None), P("dp", None, None), P(None, None), P(None, None), P(None, None), P("dp", None), P("dp"), P("dp"))
    out_specs = (P("dp"), P("dp", "seq", None), P("dp", None), P("dp", None), P("dp", None))
    return jax.shard_map(local_fn, mesh=mesh, in_specs=in_specs, out_specs=out_specs, check_vma=False)
```

```python
import functools

import jax
import jax.numpy as jnp
from jax import lax
from jax.experimental import pallas as pl
from jax.experimental.pallas import tpu as pltpu
from jax.sharding import PartitionSpec as P

NEG = -1.0e30
F32 = jnp.float32
BF16 = jnp.bfloat16
MESH = pl.DeviceIdType.MESH
LANES = 128
N_BACK = 8
VMEM_LIMIT = 57 * 2 ** 20
NT = (((1,), (1,)), ((), ()))
NN = (((1,), (0,)), ((), ()))
M_D, M_R1L, M_R1R, M_DL, M_DR, M_R2L, M_R2R, M_AL, M_AR, M_OA, M_OB, M_SC, M_SL, M_SR, M_SO = range(15)


def mm(a, b, dims=NN):
    return lax.dot_general(a, b, dims, preferred_element_type=F32)


def iota(shape, dim):
    return lax.broadcasted_iota(jnp.int32, shape, dim)


def lae(x, y):
    return jnp.maximum(x, y) + jnp.log(1.0 + jnp.exp(-jnp.abs(x - y)))


LINK_RATE, LINK_LAT, CORE_RATE, CORE_LAT = 46.6e3, 2.5, 600e3, 1.4
NEEDS = ((), (M_D,), (M_R1L, M_R1R), (M_DL, M_DR, M_R2L, M_R2R), (M_AL, M_AR), (M_OA, M_OB), (M_SC, M_SL, M_SR, M_SO))
COSTS = (.02, .25, .1, .2, .05, .05, .05)


def static_order(segs, piece, narrow):
    now, free, arrive, done, order, made = 0.0, {}, {}, {}, [], []

    def tx(kind, u, link, size):
        rate, lat = (CORE_RATE, CORE_LAT) if link == "c" else (LINK_RATE, LINK_LAT)
        begin = max(now, free.get(link, 0.0))
        free[link] = begin + size / rate
        arrive[kind, u] = free[link] + lat

    def ready(u):
        return max([arrive[k, u] for k in NEEDS[done[u]]], default=0.0)

    def step(u):
        nonlocal now
        k = done[u]
        now = max(now, ready(u)) + COSTS[k]
        ag = piece / 2 if u in narrow else piece
        if k == 0:
            tx(M_D, u, "c", 4 * piece)
        elif k == 1:
            for kind, link in ((M_R1L, "r"), (M_R1R, "l"), (M_DL, "r"), (M_DR, "l")):
                tx(kind, u, link, piece / 2)
        elif k == 2:
            tx(M_R2L, u, "r", piece / 2)
            tx(M_R2R, u, "l", piece / 2)
        elif k == 3:
            tx(M_AL, u, "r", ag)
            tx(M_AR, u, "l", ag)
            tx(M_SC, u, "c", ag)
        elif k == 4:
            tx(M_OA, u, "r", ag / 2)
            tx(M_OB, u, "l", ag / 2)
            tx(M_SL, u, "c", ag)
            tx(M_SR, u, "c", ag)
        elif k == 5:
            tx(M_SO, u, "c", ag)
        done[u] += 1
        order.append((1, u))

    left = list(range(len(segs)))
    while True:
        cand = [u for u in made if done[u] < 7]
        now_ready = [u for u in cand if ready(u) <= now]
        if now_ready:
            step(min(now_ready, key=lambda u: (done[u] > 3, made.index(u))))
        elif left:
            i = left.pop(0)
            order.append((0, i))
            now += segs[i][0]
            for u in segs[i][2]:
                made.append(u)
                done[u] = 0
        elif cand:
            step(min(cand, key=ready))
        else:
            return order


def kernel(n, n_utt, n_loc, n_pos,
           f_in, g_in, we_in, wp_in, wo_in, lab_in, flen_in, llen_in,
           loss_ref, gf_ref, gg, gd, gpt_ref,
           wot, at_s, ct_s, ht, e_s, za, zc, dz0, dz1, dz2, dz3, dad, das, dacc, pd, trs, lab_s, len_s,
           blank_r, lab_r, rs_r, gb_r, gl_r, sc_r,
           pm, recvp, sp, sr, sa, xb, yb,
           un, recvd, r1, dd, r2, t2,
           f_ref, g_ref, we_ref, wp_ref, wo_ref, lab_ref, flen_ref, llen_ref,
           lat_s, lat_r, snd, rcv, in_sem):
    loads = [pltpu.make_async_copy(src, dst, in_sem.at[q]) for q, (src, dst) in enumerate((
        (we_in, we_ref), (f_in, f_ref), (wp_in, wp_ref), (g_in, g_ref), (wo_in, wo_ref),
        (lab_in, lab_ref), (flen_in, flen_ref), (llen_in, llen_ref)))]
    for cp in loads:
        cp.start()
    me = lax.axis_index("seq")
    nchip = n // 2
    chip, core = me // 2, lax.rem(me, 2)
    k_r, k_l, k_o = lax.rem(chip + 1, nchip), lax.rem(chip + nchip - 1, nchip), lax.rem(chip + 2, nchip)
    right, left, sib = k_r * 2 + core, k_l * 2 + core, me + 1 - 2 * core
    hid = wo_ref.shape[0]
    voc = wo_ref.shape[1]
    enc = f_ref.shape[1]
    n_bt = n_utt * n_loc
    rows_t = n_utt * n_pos
    n_row = n_loc * rows_t

    barrier = pltpu.get_barrier_semaphore()
    for d in range(1, n):
        pl.semaphore_signal(barrier, inc=1, device_id={"seq": lax.rem(me + d, n)}, device_id_type=MESH)

    key_r = lax.rem(iota((n_bt, 1), 0), n_loc) * n_utt + iota((n_bt, 1), 0) // n_loc
    col = iota((1, 2 * n_bt), 1)
    key_c = (col // LANES) * n_utt + lax.rem(col, n_utt)
    pd[...] = jnp.where(key_r == key_c, 1.0, 0.0).astype(BF16)
    pc = jnp.where(key_r == iota((1, rows_t), 1), 1.0, 0.0).astype(BF16)
    loads[0].wait()
    loads[1].wait()
    at = mm(we_ref[...].T, f_ref[...], NT).astype(BF16)
    at_s[...] = mm(at, pd[...]).astype(BF16)
    loads[2].wait()
    loads[3].wait()
    ct = mm(wp_ref[...].T, g_ref[...], NT).astype(BF16)
    ct_s[...] = mm(ct, pc).astype(BF16)
    for cp in loads[4:]:
        cp.wait()
    wot[...] = wo_ref[...].T
    trs[...] = jnp.full(trs.shape, -1, jnp.int32)
    trs[0:n_pos - 1, 0:n_utt] = lab_ref[...]
    lab_t = trs[...]
    lab_alt = pltpu.roll(lab_t, n_utt, 1)
    low1 = iota((1, LANES), 1) < n_utt
    for q in range(n_pos // 2):
        lab_s[0:1, LANES * q:LANES * (q + 1)] = jnp.where(low1, lab_t[2 * q:2 * q + 1], lab_alt[2 * q + 1:2 * q + 2])
    len_s[0:1, 0:n_utt] = flen_ref[...]
    len_s[1:2, 0:n_utt] = llen_ref[...]

    fb = rows_t // 2
    n_blk = n_row // fb

    def logits(blk, z_ref):
        t = blk // 2
        off = pl.multiple_of(blk * fb, fb)
        a = at_s[:, pl.ds(pl.multiple_of(t * LANES, LANES), LANES)].astype(F32)
        c = ct_s[:, pl.ds(pl.multiple_of(lax.rem(blk, 2) * fb, fb), fb)].astype(F32)
        h = jnp.tanh(jnp.concatenate([a, a], axis=1) + c).astype(BF16)
        ht[:, pl.ds(off, fb)] = h
        z_ref[...] = mm(wot[...], h)

    def norm(blk, z_ref):
        t = blk // 2
        off = pl.multiple_of(blk * fb, fb)
        hoff = pl.multiple_of(lax.rem(blk, 2) * fb, fb)
        lab = lab_s[0:1, pl.ds(hoff, fb)]
        ch = LANES
        row = iota((ch, fb), 0)
        mx = jnp.full((8, fb), NEG, F32)
        lz = jnp.zeros((8, fb), F32)
        for i in range(voc // ch):
            z = z_ref[ch * i:ch * (i + 1), :]
            hit = jnp.where(row == lab - ch * i, z, 0.0)
            mx = jnp.maximum(mx, jnp.max(z.reshape(ch // 8, 8, fb), axis=0))
            lz = lz + jnp.sum(hit.reshape(ch // 8, 8, fb), axis=0)
        m = jnp.max(mx, axis=0, keepdims=True)
        lz = jnp.sum(lz, axis=0, keepdims=True)
        s = jnp.zeros((8, fb), F32)
        for i in range(voc // ch):
            e = jnp.exp(z_ref[ch * i:ch * (i + 1), :] - m)
            e_s[ch * i:ch * (i + 1), pl.ds(off, fb)] = e
            s = s + jnp.sum(e.reshape(ch // 8, 8, fb), axis=0)
        s = jnp.sum(s, axis=0, keepdims=True)
        lse = m + jnp.log(s)
        blank_r[pl.ds(t, 1), pl.ds(hoff, fb)] = z_ref[0:1, :] - lse
        lab_r[pl.ds(t, 1), pl.ds(hoff, fb)] = lz - lse
        rs_r[pl.ds(t, 1), pl.ds(hoff, fb)] = 1.0 / s

    def fwd(j, carry):
        logits(2 * j + 1, zc)
        norm(2 * j, za)
        logits(2 * j + 2, za)
        norm(2 * j + 1, zc)
        return carry

    logits(0, za)
    lax.fori_loop(0, n_blk // 2 - 1, fwd, 0)
    logits(n_blk - 1, zc)
    norm(n_blk - 2, za)
    norm(n_blk - 1, zc)

    lane = iota((n_loc, LANES), 1)
    low = lane < n_utt
    t_loc = iota((n_loc, LANES), 0) + me * n_loc
    len2 = jnp.where(low1, len_s[0:1, :], pltpu.roll(len_s[0:1, :], n_utt, 1))
    t_end = jnp.broadcast_to(len2, (n_loc, LANES))
    live = t_loc < t_end
    for u in range(n_pos):
        q = u // 2
        b = blank_r[:, LANES * q:LANES * (q + 1)]
        l = lab_r[:, LANES * q:LANES * (q + 1)]
        if u == n_pos - 1:
            l = jnp.full((n_loc, LANES), NEG, F32)
        if u % 2 == 0:
            l = pltpu.roll(l, n_utt, 1)
        else:
            b = pltpu.roll(b, n_utt, 1)
        pm[n_loc * u:n_loc * (u + 1), :] = jnp.where(low, jnp.where(live, b, 0.0), jnp.where(live, l, NEG))

    pl.semaphore_wait(barrier, n - 1)

    opp = k_o * 2 + core
    opp_x = k_o * 2 + 1 - core

    def lat_copy(q, src, slot, dev):
        return pltpu.make_async_remote_copy(
            src_ref=src, dst_ref=recvp.at[slot], send_sem=lat_s.at[q], recv_sem=lat_r.at[slot],
            device_id={"seq": dev}, device_id_type=MESH)

    lat_sent = [lat_copy(q, pm, me, dev) for q, dev in enumerate(
        (opp, right, left, k_r * 2 + 1 - core, k_l * 2 + 1 - core, sib))]
    for m in lat_sent:
        m.start()

    fill_lane = iota(sp.shape, 1) < n_utt
    sp[...] = jnp.where(fill_lane, 0.0, NEG)
    sr[...] = jnp.where(fill_lane, NEG, 0.0)
    u_id = iota((n_pos, LANES), 0)
    bound = jnp.where(u_id == jnp.broadcast_to(len_s[1:2, :], (n_pos, LANES)), 0.0, NEG)
    init = jnp.where(u_id == 0, 0.0, NEG)

    def put(rows, src):
        for u in range(n_pos):
            x = src[n_loc * u:n_loc * (u + 1), :]
            base = rows + (n_pos + 1) * u
            sp[pl.ds(base, n_loc, stride=n_pos), :] = x
            sr[pl.ds(base, n_loc, stride=n_pos), :] = pltpu.roll(x, n_utt, 1)

    put(me * (n_loc * n_pos), pm)
    for slot in (sib, right, left, k_r * 2 + 1 - core, k_l * 2 + 1 - core, opp, opp_x):
        lat_copy(0, pm, slot, sib).wait_recv()
        if slot is opp:
            relay = lat_copy(6, recvp.at[opp], opp, sib)
            relay.start()
            lat_sent.append(relay)
        put(slot * (n_loc * n_pos), recvp.at[slot])

    n_diag = n * n_loc + n_pos - 1

    def lattice(step, carry):
        s_a, s_b = carry
        da = pl.multiple_of(step * n_pos, n_pos)
        db = pl.multiple_of((n_diag - 1 - step) * n_pos, n_pos)
        sa[pl.ds(da, n_pos), :] = s_a
        x_a = s_a + sp[pl.ds(da, n_pos), :]
        y_a = pltpu.roll(s_a + sr[pl.ds(da, n_pos), :], 1, 0)
        x_b = s_b + sp[pl.ds(db, n_pos), :]
        y_b = pltpu.roll(s_b, n_pos - 1, 0) + sr[pl.ds(db, n_pos), :]
        xb[pl.ds(db, n_pos), :] = x_b
        yb[pl.ds(db, n_pos), :] = y_b
        return lae(x_a, y_a), lae(x_b, y_b)

    _, s_b = lax.fori_loop(0, n_diag, lattice, (init, bound))
    logp = s_b[0:1, :]
    loss_ref[...] = jnp.broadcast_to(-logp, loss_ref.shape)
    lp8 = jnp.broadcast_to(logp, (n_loc, LANES))

    gbs, gls = [], []
    for u in range(n_pos):
        rows = pl.ds(me * (n_loc * n_pos) + (n_pos + 1) * u, n_loc, stride=n_pos)
        al = sa[rows, :] - lp8
        gbs.append(jnp.where(live, jnp.exp(jnp.minimum(al + xb[rows, :], 0.0)), 0.0))
        gls.append(jnp.where(live, jnp.exp(jnp.minimum(al + yb[rows, :], 0.0)), 0.0))
    for q in range(n_pos // 2):
        ls = slice(LANES * q, LANES * (q + 1))
        gb = jnp.where(low, gbs[2 * q], pltpu.roll(gbs[2 * q + 1], n_utt, 1))
        gl = jnp.where(low, gls[2 * q], pltpu.roll(gls[2 * q + 1], n_utt, 1))
        gb_r[:, ls] = gb
        gl_r[:, ls] = gl
        sc_r[:, ls] = (gb + gl) * rs_r[:, ls]

    u_rows = un.shape[1]
    h_rows = u_rows // 2
    p_rows = h_rows // nchip
    s_rows = p_rows // 2
    mine = core * h_rows

    def msg(kind, i, src, dst, dev):
        return pltpu.make_async_remote_copy(
            src_ref=src, dst_ref=dst, send_sem=snd.at[kind, i], recv_sem=rcv.at[kind, i],
            device_id={"seq": dev}, device_id_type=MESH)

    sent = []

    def send(*args):
        m = msg(*args)
        m.start()
        sent.append(m)

    def take(kind, i, ref):
        msg(kind, i, ref, ref, sib).wait_recv()

    def hp(i, k, lo, size):
        return un.at[i, pl.ds(mine + k * p_rows + lo, size)]

    narrow = (6, 7)

    def final(i, lo, size):
        return (gd.at[i - 6] if i in narrow else gg.at[i]).at[pl.ds(lo, size)]

    def gp(i, k, lo, size):
        return final(i, mine + k * p_rows + lo, size)

    def step0(i):
        send(M_D, i, un.at[i, pl.ds((1 - core) * h_rows, h_rows)], recvd.at[i], sib)

    def step1(i):
        take(M_D, i, recvd.at[i])
        un[i, pl.ds(mine, h_rows)] += recvd[i]
        send(M_R1L, i, hp(i, k_o, 0, s_rows), r1.at[i, 0], right)
        send(M_R1R, i, hp(i, k_o, s_rows, s_rows), r1.at[i, 1], left)
        send(M_DL, i, hp(i, k_r, s_rows, s_rows), dd.at[i, 0], right)
        send(M_DR, i, hp(i, k_l, 0, s_rows), dd.at[i, 1], left)

    def step2(i):
        take(M_R1L, i, r1.at[i, 0])
        t2[i, 0] = hp(i, k_r, 0, s_rows)[...] + r1[i, 0]
        send(M_R2L, i, t2.at[i, 0], r2.at[i, 0], right)
        take(M_R1R, i, r1.at[i, 1])
        t2[i, 1] = hp(i, k_l, s_rows, s_rows)[...] + r1[i, 1]
        send(M_R2R, i, t2.at[i, 1], r2.at[i, 1], left)

    def step3(i):
        take(M_DR, i, dd.at[i, 1])
        take(M_R2L, i, r2.at[i, 0])
        res, lo = (gd, i - 6) if i in narrow else (gg, i)
        res[lo, pl.ds(mine + chip * p_rows, s_rows)] = (hp(i, chip, 0, s_rows)[...] + r2[i, 0] + dd[i, 1]).astype(res.dtype)
        take(M_DL, i, dd.at[i, 0])
        take(M_R2R, i, r2.at[i, 1])
        res[lo, pl.ds(mine + chip * p_rows + s_rows, s_rows)] = (hp(i, chip, s_rows, s_rows)[...] + r2[i, 1] + dd[i, 0]).astype(res.dtype)
        own = gp(i, chip, 0, p_rows)
        send(M_AL, i, own, own, right)
        send(M_AR, i, own, own, left)
        send(M_SC, i, own, own, sib)

    def step4(i):
        take(M_AL, i, gp(i, k_l, 0, p_rows))
        send(M_OA, i, gp(i, k_l, 0, s_rows), gp(i, k_l, 0, s_rows), right)
        take(M_AR, i, gp(i, k_r, 0, p_rows))
        send(M_OB, i, gp(i, k_r, s_rows, s_rows), gp(i, k_r, s_rows, s_rows), left)
        send(M_SL, i, gp(i, k_l, 0, p_rows), gp(i, k_l, 0, p_rows), sib)
        send(M_SR, i, gp(i, k_r, 0, p_rows), gp(i, k_r, 0, p_rows), sib)

    def step5(i):
        take(M_OA, i, gp(i, k_o, 0, s_rows))
        take(M_OB, i, gp(i, k_o, s_rows, s_rows))
        send(M_SO, i, gp(i, k_o, 0, p_rows), gp(i, k_o, 0, p_rows), sib)

    def step6(i):
        for kind, k in ((M_SC, chip), (M_SL, k_l), (M_SR, k_r), (M_SO, k_o)):
            take(kind, i, final(i, (1 - core) * h_rows + k * p_rows, p_rows))

    steps = (step0, step1, step2, step3, step4, step5, step6)
    done = [0] * 8

    def advance(*units):
        for i in units:
            steps[done[i]](i)
            done[i] += 1

    vb = u_rows // hid * LANES
    dzs = (dz0, dz1, dz2, dz3)
    kc = n_row // 4

    dc = 32

    def dz_t(i, t):
        off = pl.multiple_of(t * rows_t, rows_t)
        cols = pl.ds(off, rows_t)
        sc = sc_r[pl.ds(t, 1), :]
        gl = gl_r[pl.ds(t, 1), :]
        row = iota((dc, rows_t), 0)
        for j in range(vb // dc):
            r0 = i * vb + dc * j
            x = e_s[r0:r0 + dc, cols] * sc
            x = jnp.where(row == lab_s[0:1, :] - r0, x - gl, x)
            if r0 == 0:
                x = jnp.where(row == 0, x - gb_r[pl.ds(t, 1), :], x)
            dzs[i][dc * j:dc * (j + 1), cols] = x.astype(BF16)

    def all_dz(i):
        def body(t, carry):
            dz_t(i, t)
            return carry
        lax.fori_loop(0, n_loc, body, 0)

    def out_part(i, part):
        def body(r, carry):
            lo = pl.multiple_of(r * kc, kc)
            x = mm(ht[:, pl.ds(lo, kc)], dzs[i][:, pl.ds(lo, kc)], NT)
            for s in range(2):
                y = x[:, s * LANES:(s + 1) * LANES]
                if part == 0:
                    y = y + jnp.where(r == 0, 0.0, un[i, s * hid:(s + 1) * hid])
                else:
                    y = y + un[i, s * hid:(s + 1) * hid]
                un[i, s * hid:(s + 1) * hid] = y
            return carry
        lax.fori_loop(2 * part, 2 * part + 2, body, 0)

    def dh(blk, z_ref):
        cols = pl.ds(pl.multiple_of(blk * fb, fb), fb)
        x = mm(wo_ref[:, 0:vb], dz0[:, cols])
        for i in range(1, 4):
            x = x + mm(wo_ref[:, i * vb:(i + 1) * vb], dzs[i][:, cols])
        z_ref[0:hid, :] = x

    dr = 64

    def dp(t, half, z_ref):
        cols = pl.ds(pl.multiple_of(t * rows_t + half * fb, fb), fb)
        low = iota((dr, LANES), 1) < n_utt
        for i in range(hid // dr):
            rr = slice(dr * i, dr * (i + 1))
            h = ht[rr, cols].astype(F32)
            x = (z_ref[rr, :] * (1.0 - h * h)).astype(BF16).astype(F32)
            x0, x1 = x[:, 0:LANES], x[:, LANES:2 * LANES]
            un[6 + half, rr, :] += x0
            un[6 + half, hid + dr * i:hid + dr * (i + 1), :] += x1
            if half == 0:
                dacc[rr, :] = x0 + x1
            else:
                acc = x0 + x1 + dacc[rr, :]
                acc = acc + pltpu.roll(acc, n_utt, 1)
                dad[rr, pl.ds(pl.multiple_of(t * LANES, LANES), LANES)] = jnp.where(low, acc, 0.0).astype(BF16)

    n_back = N_BACK

    def back(part):
        if part == 0:
            un[6:8] = jnp.zeros((2, u_rows, LANES), F32)
            dh(0, za)

        def body(t, carry):
            dh(2 * t + 1, zc)
            dp(t, 0, za)
            dh(jnp.minimum(2 * t + 2, n_blk - 1), za)
            dp(t, 1, zc)
            return carry

        lax.fori_loop(part * n_loc // n_back, (part + 1) * n_loc // n_back, body, 0)

    def pred_t():
        pc2 = jnp.where(key_r == iota((1, rows_t), 1), 1.0, 0.0).astype(BF16)
        gpt_ref[...] = mm(g_ref[...].T, pc2).astype(BF16)

    def grad_w_enc():
        da = mm(pd[...], dad[...], NT).astype(BF16)
        das[...] = da
        x = mm(f_ref[...].T, da)
        for s in range(hid // LANES):
            lo, hi = s * enc, (s + 1) * enc
            first = lo
            while first < hi:
                unit = first // u_rows
                last = min(hi, (unit + 1) * u_rows)
                un[4 + unit, first - unit * u_rows:last - unit * u_rows] = x[first - lo:last - lo, s * LANES:(s + 1) * LANES]
                first = last

    def grad_enc():
        gf_ref[...] = mm(das[...], we_ref[...], NT).astype(BF16)

    segs = []
    for i in range(4):
        segs.append((.9, functools.partial(all_dz, i), ()))
        for part in range(2):
            segs.append((1.3, functools.partial(out_part, i, part), (i,) if part == 1 else ()))
    for part in range(n_back):
        segs.append((9.2 / n_back, functools.partial(back, part), (6, 7) if part == n_back - 1 else ()))
    segs.append((1.8, grad_w_enc, (4, 5)))
    segs.append((.6, grad_enc, ()))
    segs.append((.6, pred_t, ()))
    for what, i in static_order(segs, p_rows * LANES * 4, narrow):
        if what:
            advance(i)
        else:
            segs[i][1]()
    for m in sent:
        m.wait_send()
    for m in lat_sent:
        m.wait_send()


def finish(n_utt, enc, loss_in, gf_in, gg, gd, gpt, loss_ref, gf_ref, gwe_ref, gwp_ref, gwo_ref, gwp_s, sem):
    hid = gpt.shape[0]
    u_rows = gg.shape[1]
    copies = []

    def copy(src, dst):
        cp = pltpu.make_async_copy(src, dst, sem.at[len(copies)])
        cp.start()
        copies.append(cp)

    for i in range(4):
        for s in range(2):
            lo = (2 * i + s) * LANES
            copy(gg.at[i, pl.ds(s * hid, hid)], gwo_ref.at[:, pl.ds(lo, LANES)])
    copy(gf_in, gf_ref)
    for s in range(hid // LANES):
        lo, hi = s * enc, (s + 1) * enc
        first = lo
        while first < hi:
            unit = first // u_rows
            last = min(hi, (unit + 1) * u_rows)
            copy(gg.at[4 + unit, pl.ds(first - unit * u_rows, last - first)],
                 gwe_ref.at[pl.ds(first - lo, last - first), pl.ds(s * LANES, LANES)])
            first = last
    loss_ref[...] = loss_in[0:1, 0:n_utt].reshape(n_utt)
    dcb = jnp.concatenate([gd[0, 0:hid], gd[0, hid:2 * hid], gd[1, 0:hid], gd[1, hid:2 * hid]], axis=1)
    for lo in range(0, hid, 2 * LANES):
        size = min(2 * LANES, hid - lo)
        gwp_s[:, lo:lo + size] = mm(gpt[...], dcb[lo:lo + size], NT)
        copy(gwp_s.at[:, pl.ds(lo, size)], gwp_ref.at[:, pl.ds(lo, size)])
    for cp in copies:
        cp.wait()


def solution(mesh):
    n = mesh.shape["seq"]

    def local_fn(enc_out, pred_out, w_enc, w_pred, w_out, labels, frame_len, label_len):
        n_utt, n_loc, enc = enc_out.shape
        n_pos, pred = pred_out.shape[1:]
        hid, voc = w_out.shape
        assert n == 8 and 2 * n_utt == LANES and n_loc == 8 and n_pos == 8
        n_bt = n_utt * n_loc
        rows_t = n_utt * n_pos
        n_row = n_loc * rows_t
        u_rows = 2 * hid
        h_rows = u_rows // 2
        s_rows = h_rows // n
        vm = pl.BlockSpec(memory_space=pltpu.VMEM)
        anys = pl.BlockSpec(memory_space=pl.ANY)
        n_sk = (n * n_loc + n_pos) * n_pos
        vmem = pltpu.VMEM
        scratch = [
            vmem((voc, hid), BF16),
            vmem((hid, n_loc * LANES), BF16),
            vmem((hid, rows_t), BF16),
            vmem((hid, n_row), BF16),
            vmem((voc, n_row), F32),
            vmem((voc, rows_t // 2), F32),
            vmem((voc, rows_t // 2), F32),
        ] + [vmem((voc // 4, n_row), BF16)] * 4 + [
            vmem((hid, n_loc * LANES), BF16),
            vmem((n_bt, hid), BF16),
            vmem((hid, LANES), F32),
            vmem((n_bt, n_loc * LANES), BF16),
            vmem((n_pos, LANES), jnp.int32),
            vmem((8, rows_t), jnp.int32),
            vmem((8, LANES), jnp.int32),
        ] + [vmem((n_loc, rows_t), F32)] * 6 + [
            vmem((n_loc * n_pos, LANES), F32),
            vmem((n, n_loc * n_pos, LANES), F32),
        ] + [vmem((n_sk, LANES), F32)] * 5 + [
            vmem((8, u_rows, LANES), F32),
            vmem((8, h_rows, LANES), F32),
        ] + [vmem((8, 2, s_rows, LANES), F32)] * 4 + [
            vmem((n_bt, enc), BF16),
            vmem((n_utt * n_pos, pred), BF16),
            vmem((enc, hid), BF16),
            vmem((pred, hid), BF16),
            vmem((hid, voc), BF16),
            vmem((n_pos - 1, n_utt), jnp.int32),
            vmem((1, n_utt), jnp.int32),
            vmem((1, n_utt), jnp.int32),
            pltpu.SemaphoreType.DMA((n,)),
            pltpu.SemaphoreType.DMA((n,)),
            pltpu.SemaphoreType.DMA((15, 8)),
            pltpu.SemaphoreType.DMA((15, 8)),
            pltpu.SemaphoreType.DMA((8,)),
        ]
        mid = pl.pallas_call(
            functools.partial(kernel, n, n_utt, n_loc, n_pos),
            out_shape=(
                vmem((8, LANES), F32),
                vmem((n_bt, enc), BF16),
                vmem((6, u_rows, LANES), F32),
                vmem((2, u_rows, LANES), BF16),
                vmem((hid, rows_t), BF16),
            ),
            in_specs=[pl.BlockSpec(memory_space=pltpu.HBM)] * 8,
            out_specs=(vm,) * 5,
            scratch_shapes=scratch,
            compiler_params=pltpu.CompilerParams(collective_id=0, has_side_effects=True, vmem_limit_bytes=VMEM_LIMIT),
            name="rnnt",
        )(enc_out.reshape(n_bt, enc), pred_out.reshape(n_utt * n_pos, pred), w_enc, w_pred, w_out, labels.T, frame_len.reshape(1, n_utt), label_len.reshape(1, n_utt))
        mid = [pltpu.with_memory_space_constraint(x, pltpu.VMEM) for x in mid]
        loss, gf, gwe, gwp, gwo = pl.pallas_call(
            functools.partial(finish, n_utt, enc),
            out_shape=(
                jax.ShapeDtypeStruct((n_utt,), F32),
                jax.ShapeDtypeStruct((n_bt, enc), BF16),
                jax.ShapeDtypeStruct((enc, hid), F32),
                jax.ShapeDtypeStruct((pred, hid), F32),
                jax.ShapeDtypeStruct((hid, voc), F32),
            ),
            in_specs=[vm] * 5,
            out_specs=(vm, anys, anys, anys, anys),
            scratch_shapes=[vmem((pred, hid), F32), pltpu.SemaphoreType.DMA((24,))],
            compiler_params=pltpu.CompilerParams(vmem_limit_bytes=8 * 2 ** 20),
            name="finish",
        )(*mid)
        return loss, gf.reshape(n_utt, n_loc, enc), gwe, gwp, gwo

    in_specs = (P("dp", "seq", None), P("dp", None, None), P(None, None), P(None, None), P(None, None), P("dp", None), P("dp"), P("dp"))
    out_specs = (P("dp"), P("dp", "seq", None), P("dp", None), P("dp", None), P("dp", None))
    return jax.shard_map(local_fn, mesh=mesh, in_specs=in_specs, out_specs=out_specs, check_vma=False)
```

```python
import functools

import jax
import jax.numpy as jnp
from jax import lax
from jax.experimental import pallas as pl
from jax.experimental.pallas import tpu as pltpu
from jax.sharding import PartitionSpec as P

NEG = -1.0e30
F32 = jnp.float32
BF16 = jnp.bfloat16
MESH = pl.DeviceIdType.MESH
LANES = 128
N_BACK = 8
VMEM_LIMIT = 57 * 2 ** 20
NT = (((1,), (1,)), ((), ()))
NN = (((1,), (0,)), ((), ()))
M_D, M_R1L, M_R1R, M_DL, M_DR, M_R2L, M_R2R, M_AL, M_AR, M_OA, M_OB, M_SC, M_SL, M_SR, M_SO = range(15)


def mm(a, b, dims=NN):
    return lax.dot_general(a, b, dims, preferred_element_type=F32)


def iota(shape, dim):
    return lax.broadcasted_iota(jnp.int32, shape, dim)


def lae(x, y):
    return jnp.maximum(x, y) + jnp.log(1.0 + jnp.exp(-jnp.abs(x - y)))


LINK_RATE, LINK_LAT, CORE_RATE, CORE_LAT = 46.6e3, 2.5, 600e3, 1.4
NEEDS = ((), (M_D,), (M_R1L, M_R1R), (M_DL, M_DR, M_R2L, M_R2R), (M_AL, M_AR), (M_OA, M_OB), (M_SC, M_SL, M_SR, M_SO))
COSTS = (.02, .25, .1, .2, .05, .05, .05)


def static_order(segs, piece, narrow):
    now, free, arrive, done, order, made = 0.0, {}, {}, {}, [], []

    def tx(kind, u, link, size):
        rate, lat = (CORE_RATE, CORE_LAT) if link == "c" else (LINK_RATE, LINK_LAT)
        begin = max(now, free.get(link, 0.0))
        free[link] = begin + size / rate
        arrive[kind, u] = free[link] + lat

    def ready(u):
        return max([arrive[k, u] for k in NEEDS[done[u]]], default=0.0)

    def step(u):
        nonlocal now
        k = done[u]
        now = max(now, ready(u)) + COSTS[k]
        ag = piece / 2 if u in narrow else piece
        if k == 0:
            tx(M_D, u, "c", 4 * piece)
        elif k == 1:
            for kind, link in ((M_R1L, "r"), (M_R1R, "l"), (M_DL, "r"), (M_DR, "l")):
                tx(kind, u, link, piece / 2)
        elif k == 2:
            tx(M_R2L, u, "r", piece / 2)
            tx(M_R2R, u, "l", piece / 2)
        elif k == 3:
            tx(M_AL, u, "r", ag)
            tx(M_AR, u, "l", ag)
            tx(M_SC, u, "c", ag)
        elif k == 4:
            tx(M_OA, u, "r", ag / 2)
            tx(M_OB, u, "l", ag / 2)
            tx(M_SL, u, "c", ag)
            tx(M_SR, u, "c", ag)
        elif k == 5:
            tx(M_SO, u, "c", ag)
        done[u] += 1
        order.append((1, u))

    left = list(range(len(segs)))
    while True:
        cand = [u for u in made if done[u] < 7]
        now_ready = [u for u in cand if ready(u) <= now]
        if now_ready:
            step(min(now_ready, key=lambda u: (done[u] > 3, made.index(u))))
        elif left:
            i = left.pop(0)
            order.append((0, i))
            now += segs[i][0]
            for u in segs[i][2]:
                made.append(u)
                done[u] = 0
        elif cand:
            step(min(cand, key=ready))
        else:
            return order


def kernel(n, n_utt, n_loc, n_pos,
           f_in, g_in, we_in, wp_in, wo_in, lab_in, flen_in, llen_in,
           loss_ref, gf_ref, gg, gwp_ref,
           gd, wot, at_s, ct_s, ht, e_s, za, zc, dz0, dz1, dz2, dz3, dad, dacc, pd, trs, lab_s, len_s,
           blank_r, lab_r, rs_r, gb_r, gl_r, sc_r,
           pm, recvp, sp, sr, sa, xb, yb,
           un, recvd, r1, dd, r2, t2,
           f_ref, g_ref, we_ref, wp_ref, wo_ref, lab_ref, flen_ref, llen_ref,
           lat_s, lat_r, snd, rcv, in_sem):
    loads = [pltpu.make_async_copy(src, dst, in_sem.at[q]) for q, (src, dst) in enumerate((
        (we_in, we_ref), (f_in, f_ref), (wp_in, wp_ref), (g_in, g_ref), (wo_in, wo_ref),
        (lab_in, lab_ref), (flen_in, flen_ref), (llen_in, llen_ref)))]
    for cp in loads:
        cp.start()
    me = lax.axis_index("seq")
    nchip = n // 2
    chip, core = me // 2, lax.rem(me, 2)
    k_r, k_l, k_o = lax.rem(chip + 1, nchip), lax.rem(chip + nchip - 1, nchip), lax.rem(chip + 2, nchip)
    right, left, sib = k_r * 2 + core, k_l * 2 + core, me + 1 - 2 * core
    hid = wo_ref.shape[0]
    voc = wo_ref.shape[1]
    enc = f_ref.shape[1]
    n_bt = n_utt * n_loc
    rows_t = n_utt * n_pos
    n_row = n_loc * rows_t

    barrier = pltpu.get_barrier_semaphore()
    for d in range(1, n):
        pl.semaphore_signal(barrier, inc=1, device_id={"seq": lax.rem(me + d, n)}, device_id_type=MESH)

    key_r = lax.rem(iota((n_bt, 1), 0), n_loc) * n_utt + iota((n_bt, 1), 0) // n_loc
    col = iota((1, 2 * n_bt), 1)
    key_c = (col // LANES) * n_utt + lax.rem(col, n_utt)
    pd[...] = jnp.where(key_r == key_c, 1.0, 0.0).astype(BF16)
    pc = jnp.where(key_r == iota((1, rows_t), 1), 1.0, 0.0).astype(BF16)
    loads[0].wait()
    loads[1].wait()
    at = mm(we_ref[...].T, f_ref[...], NT).astype(BF16)
    at_s[...] = mm(at, pd[...]).astype(BF16)
    loads[2].wait()
    loads[3].wait()
    ct = mm(wp_ref[...].T, g_ref[...], NT).astype(BF16)
    ct_s[...] = mm(ct, pc).astype(BF16)
    for cp in loads[4:]:
        cp.wait()
    wot[...] = wo_ref[...].T
    trs[...] = jnp.full(trs.shape, -1, jnp.int32)
    trs[0:n_pos - 1, 0:n_utt] = lab_ref[...]
    lab_t = trs[...]
    lab_alt = pltpu.roll(lab_t, n_utt, 1)
    low1 = iota((1, LANES), 1) < n_utt
    for q in range(n_pos // 2):
        lab_s[0:1, LANES * q:LANES * (q + 1)] = jnp.where(low1, lab_t[2 * q:2 * q + 1], lab_alt[2 * q + 1:2 * q + 2])
    len_s[0:1, 0:n_utt] = flen_ref[...]
    len_s[1:2, 0:n_utt] = llen_ref[...]

    fb = rows_t // 2
    n_blk = n_row // fb

    def logits(blk, z_ref):
        t = blk // 2
        off = pl.multiple_of(blk * fb, fb)
        a = at_s[:, pl.ds(pl.multiple_of(t * LANES, LANES), LANES)].astype(F32)
        c = ct_s[:, pl.ds(pl.multiple_of(lax.rem(blk, 2) * fb, fb), fb)].astype(F32)
        h = jnp.tanh(jnp.concatenate([a, a], axis=1) + c).astype(BF16)
        ht[:, pl.ds(off, fb)] = h
        z_ref[...] = mm(wot[...], h)

    def norm(blk, z_ref):
        t = blk // 2
        off = pl.multiple_of(blk * fb, fb)
        hoff = pl.multiple_of(lax.rem(blk, 2) * fb, fb)
        lab = lab_s[0:1, pl.ds(hoff, fb)]
        ch = LANES
        row = iota((ch, fb), 0)
        mx = jnp.full((8, fb), NEG, F32)
        lz = jnp.zeros((8, fb), F32)
        for i in range(voc // ch):
            z = z_ref[ch * i:ch * (i + 1), :]
            hit = jnp.where(row == lab - ch * i, z, 0.0)
            mx = jnp.maximum(mx, jnp.max(z.reshape(ch // 8, 8, fb), axis=0))
            lz = lz + jnp.sum(hit.reshape(ch // 8, 8, fb), axis=0)
        m = jnp.max(mx, axis=0, keepdims=True)
        lz = jnp.sum(lz, axis=0, keepdims=True)
        s = jnp.zeros((8, fb), F32)
        for i in range(voc // ch):
            e = jnp.exp(z_ref[ch * i:ch * (i + 1), :] - m)
            e_s[ch * i:ch * (i + 1), pl.ds(off, fb)] = e
            s = s + jnp.sum(e.reshape(ch // 8, 8, fb), axis=0)
        s = jnp.sum(s, axis=0, keepdims=True)
        lse = m + jnp.log(s)
        blank_r[pl.ds(t, 1), pl.ds(hoff, fb)] = z_ref[0:1, :] - lse
        lab_r[pl.ds(t, 1), pl.ds(hoff, fb)] = lz - lse
        rs_r[pl.ds(t, 1), pl.ds(hoff, fb)] = 1.0 / s

    def fwd(j, carry):
        logits(2 * j + 1, zc)
        norm(2 * j, za)
        logits(2 * j + 2, za)
        norm(2 * j + 1, zc)
        return carry

    logits(0, za)
    lax.fori_loop(0, n_blk // 2 - 1, fwd, 0)
    logits(n_blk - 1, zc)
    norm(n_blk - 2, za)
    norm(n_blk - 1, zc)

    lane = iota((n_loc, LANES), 1)
    low = lane < n_utt
    t_loc = iota((n_loc, LANES), 0) + me * n_loc
    len2 = jnp.where(low1, len_s[0:1, :], pltpu.roll(len_s[0:1, :], n_utt, 1))
    t_end = jnp.broadcast_to(len2, (n_loc, LANES))
    live = t_loc < t_end
    for u in range(n_pos):
        q = u // 2
        b = blank_r[:, LANES * q:LANES * (q + 1)]
        l = lab_r[:, LANES * q:LANES * (q + 1)]
        if u == n_pos - 1:
            l = jnp.full((n_loc, LANES), NEG, F32)
        if u % 2 == 0:
            l = pltpu.roll(l, n_utt, 1)
        else:
            b = pltpu.roll(b, n_utt, 1)
        pm[n_loc * u:n_loc * (u + 1), :] = jnp.where(low, jnp.where(live, b, 0.0), jnp.where(live, l, NEG))

    pl.semaphore_wait(barrier, n - 1)

    opp = k_o * 2 + core
    opp_x = k_o * 2 + 1 - core

    def lat_copy(q, src, slot, dev):
        return pltpu.make_async_remote_copy(
            src_ref=src, dst_ref=recvp.at[slot], send_sem=lat_s.at[q], recv_sem=lat_r.at[slot],
            device_id={"seq": dev}, device_id_type=MESH)

    lat_sent = [lat_copy(q, pm, me, dev) for q, dev in enumerate(
        (opp, right, left, k_r * 2 + 1 - core, k_l * 2 + 1 - core, sib))]
    for m in lat_sent:
        m.start()

    fill_lane = iota(sp.shape, 1) < n_utt
    sp[...] = jnp.where(fill_lane, 0.0, NEG)
    sr[...] = jnp.where(fill_lane, NEG, 0.0)
    u_id = iota((n_pos, LANES), 0)
    bound = jnp.where(u_id == jnp.broadcast_to(len_s[1:2, :], (n_pos, LANES)), 0.0, NEG)
    init = jnp.where(u_id == 0, 0.0, NEG)

    def put(rows, src):
        for u in range(n_pos):
            x = src[n_loc * u:n_loc * (u + 1), :]
            base = rows + (n_pos + 1) * u
            sp[pl.ds(base, n_loc, stride=n_pos), :] = x
            sr[pl.ds(base, n_loc, stride=n_pos), :] = pltpu.roll(x, n_utt, 1)

    put(me * (n_loc * n_pos), pm)
    for slot in (sib, right, left, k_r * 2 + 1 - core, k_l * 2 + 1 - core, opp, opp_x):
        lat_copy(0, pm, slot, sib).wait_recv()
        if slot is opp:
            relay = lat_copy(6, recvp.at[opp], opp, sib)
            relay.start()
            lat_sent.append(relay)
        put(slot * (n_loc * n_pos), recvp.at[slot])

    n_diag = n * n_loc + n_pos - 1

    def lattice(step, carry):
        s_a, s_b = carry
        da = pl.multiple_of(step * n_pos, n_pos)
        db = pl.multiple_of((n_diag - 1 - step) * n_pos, n_pos)
        sa[pl.ds(da, n_pos), :] = s_a
        x_a = s_a + sp[pl.ds(da, n_pos), :]
        y_a = pltpu.roll(s_a + sr[pl.ds(da, n_pos), :], 1, 0)
        x_b = s_b + sp[pl.ds(db, n_pos), :]
        y_b = pltpu.roll(s_b, n_pos - 1, 0) + sr[pl.ds(db, n_pos), :]
        xb[pl.ds(db, n_pos), :] = x_b
        yb[pl.ds(db, n_pos), :] = y_b
        return lae(x_a, y_a), lae(x_b, y_b)

    _, s_b = lax.fori_loop(0, n_diag, lattice, (init, bound))
    logp = s_b[0:1, :]
    loss_ref[...] = jnp.broadcast_to(-logp, loss_ref.shape)
    lp8 = jnp.broadcast_to(logp, (n_loc, LANES))

    gbs, gls = [], []
    for u in range(n_pos):
        rows = pl.ds(me * (n_loc * n_pos) + (n_pos + 1) * u, n_loc, stride=n_pos)
        al = sa[rows, :] - lp8
        gbs.append(jnp.where(live, jnp.exp(jnp.minimum(al + xb[rows, :], 0.0)), 0.0))
        gls.append(jnp.where(live, jnp.exp(jnp.minimum(al + yb[rows, :], 0.0)), 0.0))
    for q in range(n_pos // 2):
        ls = slice(LANES * q, LANES * (q + 1))
        gb = jnp.where(low, gbs[2 * q], pltpu.roll(gbs[2 * q + 1], n_utt, 1))
        gl = jnp.where(low, gls[2 * q], pltpu.roll(gls[2 * q + 1], n_utt, 1))
        gb_r[:, ls] = gb
        gl_r[:, ls] = gl
        sc_r[:, ls] = (gb + gl) * rs_r[:, ls]

    u_rows = un.shape[1]
    h_rows = u_rows // 2
    p_rows = h_rows // nchip
    s_rows = p_rows // 2
    mine = core * h_rows

    def msg(kind, i, src, dst, dev):
        return pltpu.make_async_remote_copy(
            src_ref=src, dst_ref=dst, send_sem=snd.at[kind, i], recv_sem=rcv.at[kind, i],
            device_id={"seq": dev}, device_id_type=MESH)

    sent = []

    def send(*args):
        m = msg(*args)
        m.start()
        sent.append(m)

    def take(kind, i, ref):
        msg(kind, i, ref, ref, sib).wait_recv()

    def hp(i, k, lo, size):
        return un.at[i, pl.ds(mine + k * p_rows + lo, size)]

    narrow = (6, 7)

    def final(i, lo, size):
        return (gd.at[i - 6] if i in narrow else gg.at[i]).at[pl.ds(lo, size)]

    def gp(i, k, lo, size):
        return final(i, mine + k * p_rows + lo, size)

    def step0(i):
        send(M_D, i, un.at[i, pl.ds((1 - core) * h_rows, h_rows)], recvd.at[i], sib)

    def step1(i):
        take(M_D, i, recvd.at[i])
        un[i, pl.ds(mine, h_rows)] += recvd[i]
        send(M_R1L, i, hp(i, k_o, 0, s_rows), r1.at[i, 0], right)
        send(M_R1R, i, hp(i, k_o, s_rows, s_rows), r1.at[i, 1], left)
        send(M_DL, i, hp(i, k_r, s_rows, s_rows), dd.at[i, 0], right)
        send(M_DR, i, hp(i, k_l, 0, s_rows), dd.at[i, 1], left)

    def step2(i):
        take(M_R1L, i, r1.at[i, 0])
        t2[i, 0] = hp(i, k_r, 0, s_rows)[...] + r1[i, 0]
        send(M_R2L, i, t2.at[i, 0], r2.at[i, 0], right)
        take(M_R1R, i, r1.at[i, 1])
        t2[i, 1] = hp(i, k_l, s_rows, s_rows)[...] + r1[i, 1]
        send(M_R2R, i, t2.at[i, 1], r2.at[i, 1], left)

    def step3(i):
        take(M_DR, i, dd.at[i, 1])
        take(M_R2L, i, r2.at[i, 0])
        res, lo = (gd, i - 6) if i in narrow else (gg, i)
        res[lo, pl.ds(mine + chip * p_rows, s_rows)] = (hp(i, chip, 0, s_rows)[...] + r2[i, 0] + dd[i, 1]).astype(res.dtype)
        take(M_DL, i, dd.at[i, 0])
        take(M_R2R, i, r2.at[i, 1])
        res[lo, pl.ds(mine + chip * p_rows + s_rows, s_rows)] = (hp(i, chip, s_rows, s_rows)[...] + r2[i, 1] + dd[i, 0]).astype(res.dtype)
        own = gp(i, chip, 0, p_rows)
        send(M_AL, i, own, own, right)
        send(M_AR, i, own, own, left)
        send(M_SC, i, own, own, sib)

    def step4(i):
        take(M_AL, i, gp(i, k_l, 0, p_rows))
        send(M_OA, i, gp(i, k_l, 0, s_rows), gp(i, k_l, 0, s_rows), right)
        take(M_AR, i, gp(i, k_r, 0, p_rows))
        send(M_OB, i, gp(i, k_r, s_rows, s_rows), gp(i, k_r, s_rows, s_rows), left)
        send(M_SL, i, gp(i, k_l, 0, p_rows), gp(i, k_l, 0, p_rows), sib)
        send(M_SR, i, gp(i, k_r, 0, p_rows), gp(i, k_r, 0, p_rows), sib)

    def step5(i):
        take(M_OA, i, gp(i, k_o, 0, s_rows))
        take(M_OB, i, gp(i, k_o, s_rows, s_rows))
        send(M_SO, i, gp(i, k_o, 0, p_rows), gp(i, k_o, 0, p_rows), sib)

    def step6(i):
        for kind, k in ((M_SC, chip), (M_SL, k_l), (M_SR, k_r), (M_SO, k_o)):
            take(kind, i, final(i, (1 - core) * h_rows + k * p_rows, p_rows))

    steps = (step0, step1, step2, step3, step4, step5, step6)
    done = [0] * 8

    def advance(*units):
        for i in units:
            steps[done[i]](i)
            done[i] += 1

    vb = u_rows // hid * LANES
    dzs = (dz0, dz1, dz2, dz3)
    kc = n_row // 4

    dc = 32

    def dz_t(i, t):
        off = pl.multiple_of(t * rows_t, rows_t)
        cols = pl.ds(off, rows_t)
        sc = sc_r[pl.ds(t, 1), :]
        gl = gl_r[pl.ds(t, 1), :]
        row = iota((dc, rows_t), 0)
        for j in range(vb // dc):
            r0 = i * vb + dc * j
            x = e_s[r0:r0 + dc, cols] * sc
            x = jnp.where(row == lab_s[0:1, :] - r0, x - gl, x)
            if r0 == 0:
                x = jnp.where(row == 0, x - gb_r[pl.ds(t, 1), :], x)
            dzs[i][dc * j:dc * (j + 1), cols] = x.astype(BF16)

    def all_dz(i):
        def body(t, carry):
            dz_t(i, t)
            return carry
        lax.fori_loop(0, n_loc, body, 0)

    def out_part(i, part):
        def body(r, carry):
            lo = pl.multiple_of(r * kc, kc)
            x = mm(ht[:, pl.ds(lo, kc)], dzs[i][:, pl.ds(lo, kc)], NT)
            for s in range(2):
                y = x[:, s * LANES:(s + 1) * LANES]
                if part == 0:
                    y = y + jnp.where(r == 0, 0.0, un[i, s * hid:(s + 1) * hid])
                else:
                    y = y + un[i, s * hid:(s + 1) * hid]
                un[i, s * hid:(s + 1) * hid] = y
            return carry
        lax.fori_loop(2 * part, 2 * part + 2, body, 0)

    def dh(blk, z_ref):
        cols = pl.ds(pl.multiple_of(blk * fb, fb), fb)
        x = mm(wo_ref[:, 0:vb], dz0[:, cols])
        for i in range(1, 4):
            x = x + mm(wo_ref[:, i * vb:(i + 1) * vb], dzs[i][:, cols])
        z_ref[0:hid, :] = x

    dr = 64

    def dp(t, half, z_ref):
        cols = pl.ds(pl.multiple_of(t * rows_t + half * fb, fb), fb)
        low = iota((dr, LANES), 1) < n_utt
        for i in range(hid // dr):
            rr = slice(dr * i, dr * (i + 1))
            h = ht[rr, cols].astype(F32)
            x = (z_ref[rr, :] * (1.0 - h * h)).astype(BF16).astype(F32)
            x0, x1 = x[:, 0:LANES], x[:, LANES:2 * LANES]
            un[6 + half, rr, :] += x0
            un[6 + half, hid + dr * i:hid + dr * (i + 1), :] += x1
            if half == 0:
                dacc[rr, :] = x0 + x1
            else:
                acc = x0 + x1 + dacc[rr, :]
                acc = acc + pltpu.roll(acc, n_utt, 1)
                dad[rr, pl.ds(pl.multiple_of(t * LANES, LANES), LANES)] = jnp.where(low, acc, 0.0).astype(BF16)

    n_back = N_BACK

    def back(part):
        if part == 0:
            un[6:8] = jnp.zeros((2, u_rows, LANES), F32)
            dh(0, za)

        def body(t, carry):
            dh(2 * t + 1, zc)
            dp(t, 0, za)
            dh(jnp.minimum(2 * t + 2, n_blk - 1), za)
            dp(t, 1, zc)
            return carry

        lax.fori_loop(part * n_loc // n_back, (part + 1) * n_loc // n_back, body, 0)

    def pred_t():
        pc2 = jnp.where(key_r == iota((1, rows_t), 1), 1.0, 0.0).astype(BF16)
        ct_s[...] = mm(g_ref[...].T, pc2).astype(BF16)

    def grad_w_enc():
        da = mm(pd[...], dad[...], NT).astype(BF16)
        at_s[0:n_bt, 0:hid] = da
        x = mm(f_ref[...].T, da)
        for s in range(hid // LANES):
            lo, hi = s * enc, (s + 1) * enc
            first = lo
            while first < hi:
                unit = first // u_rows
                last = min(hi, (unit + 1) * u_rows)
                un[4 + unit, first - unit * u_rows:last - unit * u_rows] = x[first - lo:last - lo, s * LANES:(s + 1) * LANES]
                first = last

    def grad_w_pred():
        dcb = jnp.concatenate([gd[0, 0:hid], gd[0, hid:2 * hid], gd[1, 0:hid], gd[1, hid:2 * hid]], axis=1)
        gwp_ref[...] = mm(ct_s[...], dcb, NT)

    def grad_enc():
        gf_ref[...] = mm(at_s[0:n_bt, 0:hid], we_ref[...], NT).astype(BF16)

    segs = []
    for i in range(4):
        segs.append((.9, functools.partial(all_dz, i), ()))
        for part in range(2):
            segs.append((1.3, functools.partial(out_part, i, part), (i,) if part == 1 else ()))
    for part in range(n_back):
        segs.append((9.2 / n_back, functools.partial(back, part), (6, 7) if part == n_back - 1 else ()))
    segs.append((1.8, grad_w_enc, (4, 5)))
    segs.append((.6, grad_enc, ()))
    segs.append((.6, pred_t, ()))
    for what, i in static_order(segs, p_rows * LANES * 4, narrow):
        if what:
            advance(i)
            if i in narrow and done[6] == done[7] == 7:
                grad_w_pred()
        else:
            segs[i][1]()
    for m in sent:
        m.wait_send()
    for m in lat_sent:
        m.wait_send()


def finish(n_utt, enc, loss_in, gf_in, gg, gwp_in, loss_ref, gf_ref, gwe_ref, gwp_ref, gwo_ref, sem):
    hid = gwp_in.shape[1]
    u_rows = gg.shape[1]
    copies = []

    def copy(src, dst):
        cp = pltpu.make_async_copy(src, dst, sem.at[len(copies)])
        cp.start()
        copies.append(cp)

    for i in range(4):
        for s in range(2):
            lo = (2 * i + s) * LANES
            copy(gg.at[i, pl.ds(s * hid, hid)], gwo_ref.at[:, pl.ds(lo, LANES)])
    copy(gf_in, gf_ref)
    copy(gwp_in, gwp_ref)
    for s in range(hid // LANES):
        lo, hi = s * enc, (s + 1) * enc
        first = lo
        while first < hi:
            unit = first // u_rows
            last = min(hi, (unit + 1) * u_rows)
            copy(gg.at[4 + unit, pl.ds(first - unit * u_rows, last - first)],
                 gwe_ref.at[pl.ds(first - lo, last - first), pl.ds(s * LANES, LANES)])
            first = last
    loss_ref[...] = loss_in[0:1, 0:n_utt].reshape(n_utt)
    for cp in copies:
        cp.wait()


def solution(mesh):
    n = mesh.shape["seq"]

    def local_fn(enc_out, pred_out, w_enc, w_pred, w_out, labels, frame_len, label_len):
        n_utt, n_loc, enc = enc_out.shape
        n_pos, pred = pred_out.shape[1:]
        hid, voc = w_out.shape
        assert n == 8 and 2 * n_utt == LANES and n_loc == 8 and n_pos == 8
        n_bt = n_utt * n_loc
        rows_t = n_utt * n_pos
        n_row = n_loc * rows_t
        u_rows = 2 * hid
        h_rows = u_rows // 2
        s_rows = h_rows // n
        vm = pl.BlockSpec(memory_space=pltpu.VMEM)
        anys = pl.BlockSpec(memory_space=pl.ANY)
        n_sk = (n * n_loc + n_pos) * n_pos
        vmem = pltpu.VMEM
        scratch = [
            vmem((2, u_rows, LANES), BF16),
            vmem((voc, hid), BF16),
            vmem((hid, n_loc * LANES), BF16),
            vmem((hid, rows_t), BF16),
            vmem((hid, n_row), BF16),
            vmem((voc, n_row), F32),
            vmem((voc, rows_t // 2), F32),
            vmem((voc, rows_t // 2), F32),
        ] + [vmem((voc // 4, n_row), BF16)] * 4 + [
            vmem((hid, n_loc * LANES), BF16),
            vmem((hid, LANES), F32),
            vmem((n_bt, n_loc * LANES), BF16),
            vmem((n_pos, LANES), jnp.int32),
            vmem((8, rows_t), jnp.int32),
            vmem((8, LANES), jnp.int32),
        ] + [vmem((n_loc, rows_t), F32)] * 6 + [
            vmem((n_loc * n_pos, LANES), F32),
            vmem((n, n_loc * n_pos, LANES), F32),
        ] + [vmem((n_sk, LANES), F32)] * 5 + [
            vmem((8, u_rows, LANES), F32),
            vmem((8, h_rows, LANES), F32),
        ] + [vmem((8, 2, s_rows, LANES), F32)] * 4 + [
            vmem((n_bt, enc), BF16),
            vmem((n_utt * n_pos, pred), BF16),
            vmem((enc, hid), BF16),
            vmem((pred, hid), BF16),
            vmem((hid, voc), BF16),
            vmem((n_pos - 1, n_utt), jnp.int32),
            vmem((1, n_utt), jnp.int32),
            vmem((1, n_utt), jnp.int32),
            pltpu.SemaphoreType.DMA((n,)),
            pltpu.SemaphoreType.DMA((n,)),
            pltpu.SemaphoreType.DMA((15, 8)),
            pltpu.SemaphoreType.DMA((15, 8)),
            pltpu.SemaphoreType.DMA((8,)),
        ]
        mid = pl.pallas_call(
            functools.partial(kernel, n, n_utt, n_loc, n_pos),
            out_shape=(
                vmem((8, LANES), F32),
                vmem((n_bt, enc), BF16),
                vmem((6, u_rows, LANES), F32),
                vmem((pred, hid), F32),
            ),
            in_specs=[pl.BlockSpec(memory_space=pltpu.HBM)] * 8,
            out_specs=(vm,) * 4,
            scratch_shapes=scratch,
            compiler_params=pltpu.CompilerParams(collective_id=0, has_side_effects=True, vmem_limit_bytes=VMEM_LIMIT),
            name="rnnt",
        )(enc_out.reshape(n_bt, enc), pred_out.reshape(n_utt * n_pos, pred), w_enc, w_pred, w_out, labels.T, frame_len.reshape(1, n_utt), label_len.reshape(1, n_utt))
        mid = [pltpu.with_memory_space_constraint(x, pltpu.VMEM) for x in mid]
        loss, gf, gwe, gwp, gwo = pl.pallas_call(
            functools.partial(finish, n_utt, enc),
            out_shape=(
                jax.ShapeDtypeStruct((n_utt,), F32),
                jax.ShapeDtypeStruct((n_bt, enc), BF16),
                jax.ShapeDtypeStruct((enc, hid), F32),
                jax.ShapeDtypeStruct((pred, hid), F32),
                jax.ShapeDtypeStruct((hid, voc), F32),
            ),
            in_specs=[vm] * 4,
            out_specs=(vm, anys, anys, anys, anys),
            scratch_shapes=[pltpu.SemaphoreType.DMA((24,))],
            compiler_params=pltpu.CompilerParams(vmem_limit_bytes=2 ** 20),
            name="finish",
        )(*mid)
        return loss, gf.reshape(n_utt, n_loc, enc), gwe, gwp, gwo

    in_specs = (P("dp", "seq", None), P("dp", None, None), P(None, None), P(None, None), P(None, None), P("dp", None), P("dp"), P("dp"))
    out_specs = (P("dp"), P("dp", "seq", None), P("dp", None), P("dp", None), P("dp", None))
    return jax.shard_map(local_fn, mesh=mesh, in_specs=in_specs, out_specs=out_specs, check_vma=False)
```
